256 devices in a mesh: col: 8 (over y, core), row: 32 (over z, x).
Axes of the slice: x: 4, y: 4, z: 8, core: 2. Of those that a mesh axis runs over, the one named last changes fastest.
Arguments:
- column_table: float32 [262144, 512], P('row', 'col'), may hold values from -3 to 3
- bag_rows: int32 [1024, 32], P('row'), may hold values from 0 to 262143
Outputs:
- row_table: float32 [32, 8192, 512], P(None, ('col', 'row'))
- pooled: float32 [1024, 512], P('row', 'col')
The draws below stay inside these ranges and needn't reach their ends.
Inputs may be any that keep to these rules, and one draw needn't show every extreme that they name: `bag_rows`: row indices of the table; a few rows are named far more often than the rest.
All inputs are finite; a program needn't handle non-finite values.
Results may differ from the reference program's by a relative error of at most 0.000078.
Values sent between devices are 32-bit elements; how exact they have to be, the bound alone decides.
A program may use at most 64 MiB of HBM per device.

```python
import math
import jax
import jax.numpy as jnp
import numpy as np

E = 512
BAG_LEN = 32
ROWS = 262144
GROUPS = 32
BLOCK = 8192
BAGS = 1024


def place_ends(drawn, own_key, low, top_value):
    place = [jax.random.randint(jax.random.fold_in(own_key, axis), (), 0, length) for axis, length in enumerate(drawn.shape)]
    longest = drawn.shape.index(max(drawn.shape))
    next_to = place[:longest] + [(place[longest] + 1) % drawn.shape[longest]] + place[longest + 1:]
    return drawn.at[tuple(place)].set(low).at[tuple(next_to)].set(top_value)


def block_scale(rng, shape, pieces, low, largest):
    gain = 1.0
    for position, shards_of in pieces:
        draws = jax.random.uniform(jax.random.fold_in(jax.random.fold_in(rng, 6), position), (shards_of,), jnp.float32, low / len(pieces), largest / len(pieces))
        gain = gain * jnp.repeat(jnp.exp(draws), shape[position] // shards_of).reshape((-1,) + (1,) * (len(shape) - 1 - position))
    return gain


def wide_ids(own_key, shape, amount, skew):
    portions = [min(1 << octave, amount + 1 - (1 << octave)) * (1 << 20) // math.isqrt((1 << octave) ** skew) + 1 for octave in range((amount + 1).bit_length()) if 1 << octave <= amount]
    scale = 1 + sum(portions) // (1 << 30)
    table = np.cumsum(np.array([max(1, weight // scale) for weight in portions]))
    lot = jax.random.randint(jax.random.fold_in(own_key, 1), shape, 0, int(table[len(portions) - 1]))
    start = jnp.left_shift(1, jnp.searchsorted(jnp.asarray(table, jnp.int32), lot, side="right").astype(jnp.int32))
    rank = start - 1 + jax.random.randint(jax.random.fold_in(own_key, 4), shape, 0, 1 << 30) % jnp.minimum(start, amount + 1 - start)
    return jax.random.permutation(jax.random.fold_in(own_key, 2), amount)[rank].astype(jnp.int32)


def centred(stream_key, shape, scale, bound, cuts=(), dtype=jnp.bfloat16):
    level = block_scale(stream_key, shape, cuts, -0.22, 0.18) if cuts else 1.0
    entries = jax.random.normal(stream_key, shape, jnp.float32) * scale * level
    return jnp.minimum(jnp.maximum(entries, -bound), bound).astype(dtype)


def setup_inputs(seed: int = 0) -> dict:
    key_list = jax.random.split(jax.random.key(seed), 3)
    column_table = centred(key_list[0], (ROWS, E), 0.2, 3.0, ((0, 32), (1, 8)), jnp.float32)
    bag_rows = place_ends(wide_ids(key_list[1], (BAGS, BAG_LEN), ROWS, 2), jax.random.fold_in(key_list[1], 3), 0, ROWS - 1).astype(jnp.int32)
    return dict(column_table=column_table, bag_rows=bag_rows)


def reference(column_table, bag_rows):
    row_table = column_table.reshape(GROUPS, BLOCK, E)
    picked = jnp.take(column_table, bag_rows.reshape(-1), axis=0).reshape(BAGS, BAG_LEN, E)
    pooled = jnp.sum(picked.astype(jnp.float32), axis=1)
    return row_table, pooled
```

```python
import functools

import jax
import jax.numpy as jnp
from jax import lax
from jax.experimental import pallas as pl
from jax.experimental.pallas import tpu as pltpu
from jax.sharding import PartitionSpec as P

MESH = pl.DeviceIdType.MESH
LANES = 128
BAG_LEN = 32


def kernel(
    zn, xn, span, table_ref, bags_ref, out_ref, pooled_ref,
    raw, flat, ids, near, part2, part, x_in, held, z_in, spot,
    load_sem, pair_send, pair_recv, ids_send, ids_recv, move_send, move_recv,
    x_send, x_recv, z_send, z_recv, spot_sem, own_sem,
):
    rows = zn * xn
    half, length = table_ref.shape
    width = rows * span
    chunks = length // width
    yn = chunks // 2
    col = lax.axis_index("col")
    row = lax.axis_index("row")
    y, core = col // 2, col % 2
    z, x = row // xn, row % xn
    sibling = y * 2 + (1 - core)

    def chunk_at(i, parity):
        c = lax.rem(y + i, yn) * 2 + parity
        return c, pl.ds(pl.multiple_of(c * width, LANES), width)

    def local_load(n):
        c, lanes = chunk_at(n % yn, core if n < yn else 1 - core)
        mine = pl.ds(pl.multiple_of(core * half, 8), half)
        return pltpu.make_async_copy(table_ref.at[:, lanes], raw.at[mine, lanes], load_sem.at[n])

    def pair_copy(n):
        c, lanes = chunk_at(n % yn, 1 - core if n < yn else core)
        mine = pl.ds(pl.multiple_of(core * half, 8), half)
        return pltpu.make_async_remote_copy(
            src_ref=table_ref.at[:, lanes], dst_ref=raw.at[mine, lanes],
            send_sem=pair_send.at[n], recv_sem=pair_recv.at[n],
            device_id=(sibling, row), device_id_type=MESH,
        )

    for n in range(chunks):
        pair_copy(n).start()
        local_load(n).start()

    bags = bags_ref[...]
    eighth = bags.shape[0] // 4
    own_ids = pl.ds(pl.multiple_of(row * eighth, 8), eighth)
    ids[own_ids, :] = jnp.concatenate([bags[q * eighth : (q + 1) * eighth] for q in range(4)], axis=1)
    flat[pl.ds(length, 8), :] = jnp.zeros((8, LANES), jnp.float32)

    def transpose(n):
        c, lanes = chunk_at(n % yn, core if n < yn else 1 - core)
        local_load(n).wait()
        pair_copy(n).wait_recv()

        def step(t, carry):
            at = pl.ds(pl.multiple_of(c * width + t * LANES, LANES), LANES)
            flat[at, :] = raw[:, at].T
            return carry

        lax.fori_loop(0, width // LANES, step, 0)

    def block(c, rr):
        return flat.at[pl.ds(pl.multiple_of(c * width + rr * span, 8), span)]

    landing = out_ref.at[row, :, pl.ds(pl.multiple_of(y * LANES, LANES), LANES)]

    def send_blocks(n):
        c, _ = chunk_at(n, core)

        def step(t, carry):
            rr = lax.rem(z + t // xn, zn) * xn + lax.rem(x + t % xn, xn)
            pltpu.make_async_remote_copy(
                src_ref=block(c, rr), dst_ref=landing, send_sem=move_send, recv_sem=move_recv,
                device_id=(c, rr), device_id_type=MESH,
            ).start()
            return carry

        lax.fori_loop(1 if n == 0 else 0, rows, step, 0)

    def send_ids(t, carry):
        rr = lax.rem(row + t, rows)
        pltpu.make_async_remote_copy(
            src_ref=ids.at[own_ids], dst_ref=ids.at[own_ids], send_sem=ids_send, recv_sem=ids_recv,
            device_id=(col, rr), device_id_type=MESH,
        ).start()
        return carry

    transpose(0)
    lax.fori_loop(1, rows, send_ids, 0)
    for n in range(yn):
        if n + 1 < yn:
            transpose(n + 1)
        else:
            transpose(yn)
        send_blocks(n)
    own = pltpu.make_async_copy(block(col, row), landing, own_sem)
    own.start()
    for n in range(yn + 1, chunks):
        transpose(n)

    others = (rows - 1) * eighth
    pltpu.make_async_copy(ids.at[pl.ds(0, others)], ids.at[pl.ds(0, others)], ids_recv).wait()
    every = ids[...]
    near[...] = jnp.where(every // length == row, every % length, length)
    to_scalar = pltpu.make_async_copy(near, spot, spot_sem)
    to_scalar.start()
    to_scalar.wait()

    def gather(t, carry):
        for q in range(2):
            sums = [None] * 4
            for l in range(BAG_LEN):
                at = spot[t, core * (2 * BAG_LEN) + q * BAG_LEN + l]
                value = flat[pl.ds(at, 1), :]
                sums[l % 4] = value if sums[l % 4] is None else sums[l % 4] + value
            part2[q, pl.ds(t, 1), :] = (sums[0] + sums[1]) + (sums[2] + sums[3])
        return carry

    lax.fori_loop(0, rows * eighth, gather, 0)

    low = lax.broadcasted_iota(jnp.int32, (8, LANES), 1) < half

    def split(s, carry):
        at = pl.ds(pl.multiple_of(s * 8, 8), 8)
        first, second = part2[0, at, :], part2[1, at, :]
        part[s % xn, s // xn, 0] = jnp.where(low, first, pltpu.roll(second, half, 1))
        part[s % xn, s // xn, 1] = jnp.where(low, pltpu.roll(first, half, 1), second)
        return carry

    lax.fori_loop(0, rows, split, 0)

    for d in range(1, xn):
        xx = lax.rem(x + d, xn)
        pltpu.make_async_remote_copy(
            src_ref=part.at[xx], dst_ref=x_in.at[x], send_sem=x_send, recv_sem=x_recv,
            device_id=(col, z * xn + xx), device_id_type=MESH,
        ).start()
    x_rest = part.at[pl.ds(0, xn - 1)]
    pltpu.make_async_copy(x_rest, x_rest, x_recv).wait()
    total = part[x]
    for d in range(1, xn):
        total = total + x_in[lax.rem(x + d, xn)]
    held[...] = total

    for d in range(zn):
        zz = lax.rem(z + d, zn)
        for e in range(2):
            if d == 0 and e == 0:
                continue
            kk = core if e == 0 else 1 - core
            pltpu.make_async_remote_copy(
                src_ref=held.at[zz, kk], dst_ref=z_in.at[z * 2 + core], send_sem=z_send, recv_sem=z_recv,
                device_id=(y * 2 + kk, zz * xn + x), device_id_type=MESH,
            ).start()
    z_in[z * 2 + core] = held[z, core]
    z_rest = z_in.at[pl.ds(0, 2 * zn - 1)]
    pltpu.make_async_copy(z_rest, z_rest, z_recv).wait()
    for k in range(2):
        total = z_in[k]
        for d in range(1, zn):
            total = total + z_in[d * 2 + k]
        pooled_ref[pl.ds(k * 16, 8), :] = total[:, :half]
        pooled_ref[pl.ds(k * 16 + 8, 8), :] = pltpu.roll(total, half, 1)[:, :half]

    own.wait()
    moved = flat.at[pl.ds(0, (yn * rows - 1) * span)]
    pltpu.make_async_copy(moved, moved, move_recv).wait()
    pltpu.make_async_copy(moved, moved, move_send).wait()
    sent_ids = ids.at[pl.ds(0, others)]
    pltpu.make_async_copy(sent_ids, sent_ids, ids_send).wait()
    pltpu.make_async_copy(x_rest, x_rest, x_send).wait()
    pltpu.make_async_copy(z_rest, z_rest, z_send).wait()
    for n in range(chunks):
        pair_copy(n).wait_send()


def per_device(zn, xn, column_table, bag_rows):
    rows = zn * xn
    chunks = lax.axis_size("col")
    length, half = column_table.shape
    span = length // (rows * chunks)
    f32 = jnp.float32
    dma = pltpu.SemaphoreType.DMA
    row_table, pooled = pl.pallas_call(
        functools.partial(kernel, zn, xn, span),
        out_shape=[
            jax.ShapeDtypeStruct((rows, span, half * chunks), f32),
            jax.ShapeDtypeStruct((bag_rows.shape[0], half), f32),
        ],
        in_specs=[pl.BlockSpec(memory_space=pl.ANY), pl.BlockSpec(memory_space=pltpu.VMEM)],
        out_specs=[pl.BlockSpec(memory_space=pl.ANY), pl.BlockSpec(memory_space=pltpu.VMEM)],
        scratch_shapes=[
            pltpu.VMEM((2 * half, length), f32),
            pltpu.VMEM((length + 8, LANES), f32),
            pltpu.VMEM((rows * 8, LANES), jnp.int32),
            pltpu.VMEM((rows * 8, LANES), jnp.int32),
            pltpu.VMEM((2, rows * 8, LANES), f32),
            pltpu.VMEM((xn, zn, 2, 8, LANES), f32),
            pltpu.VMEM((xn, zn, 2, 8, LANES), f32),
            pltpu.VMEM((zn, 2, 8, LANES), f32),
            pltpu.VMEM((zn * 2, 8, LANES), f32),
            pltpu.SMEM((rows * 8, LANES), jnp.int32),
            dma((chunks,)), dma((chunks,)), dma((chunks,)),
            dma, dma, dma, dma, dma, dma, dma, dma, dma, dma,
        ],
        compiler_params=pltpu.CompilerParams(has_side_effects=True, vmem_limit_bytes=40 * 1024 * 1024),
    )(column_table.T, bag_rows)
    return row_table, pooled


def solution(mesh):
    rows = mesh.shape["row"]
    xn = 4 if rows == 32 else 2
    return jax.shard_map(
        functools.partial(per_device, rows // xn, xn),
        mesh=mesh,
        in_specs=(P("row", "col"), P("row", None)),
        out_specs=(P(None, ("col", "row"), None), P("row", "col")),
        check_vma=False,
    )
```

```python
import functools

import jax
import jax.numpy as jnp
from jax import lax
from jax.experimental import pallas as pl
from jax.experimental.pallas import tpu as pltpu
from jax.sharding import PartitionSpec as P

MESH = pl.DeviceIdType.MESH
LANES = 128
BAG_LEN = 32


def kernel(
    zn, xn, span, table_ref, bags_ref, out_ref, pooled_ref,
    raw, flat, bags, ids, near, part2, part, x_in, held, z_in, spot,
    load_sem, pair_send, pair_recv, ids_send, ids_recv, move_send, move_recv,
    x_send, x_recv, z_send, z_recv, spot_sem, own_sem, bags_sem,
):
    rows = zn * xn
    half, length = table_ref.shape
    width = rows * span
    chunks = length // width
    yn = chunks // 2
    col = lax.axis_index("col")
    row = lax.axis_index("row")
    y, core = col // 2, col % 2
    z, x = row // xn, row % xn
    sibling = y * 2 + (1 - core)
    away = sorted(range(1, zn), key=lambda d: -min(d, zn - d))

    barrier = pltpu.get_barrier_semaphore()

    def greet(c, rr):
        pl.semaphore_signal(barrier, inc=1, device_id=(c, rr), device_id_type=MESH)

    def greet_plane(i, carry):
        c = lax.rem(y + i, yn) * 2 + core
        for dx in range(xn):
            xx = lax.rem(x + dx, xn)
            for dz in away + ([0] if dx else []):
                greet(c, lax.rem(z + dz, zn) * xn + xx)
        return carry

    greet(sibling, row)
    lax.fori_loop(0, yn, greet_plane, 0)
    for dz in away:
        greet(sibling, lax.rem(z + dz, zn) * xn + x)
    for i in range(1, yn):
        greet(lax.rem(y + i, yn) * 2 + core, row)

    def chunk_at(i, parity):
        c = lax.rem(y + i, yn) * 2 + parity
        return c, pl.ds(pl.multiple_of(c * width, LANES), width)

    def local_load(n):
        c, lanes = chunk_at(n % yn, core if n < yn else 1 - core)
        mine = pl.ds(pl.multiple_of(core * half, 8), half)
        return pltpu.make_async_copy(table_ref.at[:, lanes], raw.at[mine, lanes], load_sem.at[n])

    def pair_copy(n):
        c, lanes = chunk_at(n % yn, 1 - core if n < yn else core)
        mine = pl.ds(pl.multiple_of(core * half, 8), half)
        return pltpu.make_async_remote_copy(
            src_ref=table_ref.at[:, lanes], dst_ref=raw.at[mine, lanes],
            send_sem=pair_send.at[n], recv_sem=pair_recv.at[n],
            device_id=(sibling, row), device_id_type=MESH,
        )

    load_bags = pltpu.make_async_copy(bags_ref, bags, bags_sem)
    load_bags.start()
    for n in range(chunks):
        local_load(n).start()

    load_bags.wait()
    eighth = bags.shape[0] // 4
    own_ids = pl.ds(pl.multiple_of(row * eighth, 8), eighth)
    ids[own_ids, :] = jnp.concatenate([bags[q * eighth : (q + 1) * eighth, :] for q in range(4)], axis=1)
    pl.semaphore_wait(barrier, yn * rows - 1 + zn)
    for n in range(chunks):
        pair_copy(n).start()
    flat[pl.ds(length, 8), :] = jnp.zeros((8, LANES), jnp.float32)

    def transpose(n):
        c, lanes = chunk_at(n % yn, core if n < yn else 1 - core)
        local_load(n).wait()
        pair_copy(n).wait_recv()

        def step(t, carry):
            at = pl.ds(pl.multiple_of(c * width + t * LANES, LANES), LANES)
            flat[at, :] = raw[:, at].T
            return carry

        lax.fori_loop(0, width // LANES, step, 0)

    def block(c, rr):
        return flat.at[pl.ds(pl.multiple_of(c * width + rr * span, 8), span)]

    landing = out_ref.at[row, :, pl.ds(pl.multiple_of(y * LANES, LANES), LANES)]

    def send_blocks(n):
        c, _ = chunk_at(n, core)

        def send(rr):
            pltpu.make_async_remote_copy(
                src_ref=block(c, rr), dst_ref=landing, send_sem=move_send, recv_sem=move_recv,
                device_id=(c, rr), device_id_type=MESH,
            ).start()

        def step(dx, carry):
            xx = lax.rem(x + dx, xn)
            for dz in away:
                send(lax.rem(z + dz, zn) * xn + xx)
            return carry

        def step_near(dx, carry):
            send(z * xn + lax.rem(x + dx, xn))
            return carry

        lax.fori_loop(0, xn, step, 0)
        lax.fori_loop(1 if n == 0 else 0, xn, step_near, 0)

    def send_ids(t, carry):
        rr = lax.rem(row + t, rows)
        pltpu.make_async_remote_copy(
            src_ref=ids.at[own_ids], dst_ref=ids.at[own_ids], send_sem=ids_send, recv_sem=ids_recv,
            device_id=(col, rr), device_id_type=MESH,
        ).start()
        return carry

    lax.fori_loop(1, rows, send_ids, 0)
    transpose(0)
    transpose(1)
    send_blocks(0)
    transpose(2 % chunks)
    send_blocks(1)
    for n in range(3, chunks):
        transpose(n)

    others = (rows - 1) * eighth
    pltpu.make_async_copy(ids.at[pl.ds(0, others)], ids.at[pl.ds(0, others)], ids_recv).wait()
    every = ids[...]
    every = jnp.where(every // length == row, every % length, length)
    near[...] = jnp.where(core == 0, every, pltpu.roll(every, LANES // 2, 1))
    to_scalar = pltpu.make_async_copy(near, spot, spot_sem)
    to_scalar.start()
    to_scalar.wait()

    def gather(t, carry):
        for q in range(2):
            sums = [None] * 4
            for l in range(BAG_LEN):
                at = spot[t, q * BAG_LEN + l]
                value = flat[pl.ds(at, 1), :]
                sums[l % 4] = value if sums[l % 4] is None else sums[l % 4] + value
            part2[q, pl.ds(t, 1), :] = (sums[0] + sums[1]) + (sums[2] + sums[3])
        return carry

    lax.fori_loop(0, rows * eighth, gather, 0)

    low = lax.broadcasted_iota(jnp.int32, (8, LANES), 1) < half

    def split(s, carry):
        at = pl.ds(pl.multiple_of(s * 8, 8), 8)
        first, second = part2[0, at, :], part2[1, at, :]
        part[s % xn, s // xn, 0] = jnp.where(low, first, pltpu.roll(second, half, 1))
        part[s % xn, s // xn, 1] = jnp.where(low, pltpu.roll(first, half, 1), second)
        return carry

    lax.fori_loop(0, rows, split, 0)

    for d in range(1, xn):
        xx = lax.rem(x + d, xn)
        pltpu.make_async_remote_copy(
            src_ref=part.at[xx], dst_ref=x_in.at[x], send_sem=x_send, recv_sem=x_recv,
            device_id=(col, z * xn + xx), device_id_type=MESH,
        ).start()
    for n in range(2, yn - 1):
        send_blocks(n)
    x_rest = part.at[pl.ds(0, xn - 1)]
    pltpu.make_async_copy(x_rest, x_rest, x_recv).wait()
    total = part[x]
    for d in range(1, xn):
        total = total + x_in[lax.rem(x + d, xn)]
    held[...] = total

    for d in range(zn):
        zz = lax.rem(z + d, zn)
        for e in range(2):
            if d == 0 and e == 0:
                continue
            kk = core if e == 0 else 1 - core
            pltpu.make_async_remote_copy(
                src_ref=held.at[zz, kk], dst_ref=z_in.at[z * 2 + core], send_sem=z_send, recv_sem=z_recv,
                device_id=(y * 2 + kk, zz * xn + x), device_id_type=MESH,
            ).start()
    if yn > 2:
        send_blocks(yn - 1)
    own = pltpu.make_async_copy(block(col, row), landing, own_sem)
    own.start()
    z_in[z * 2 + core] = held[z, core]
    z_rest = z_in.at[pl.ds(0, 2 * zn - 1)]
    pltpu.make_async_copy(z_rest, z_rest, z_recv).wait()
    for k in range(2):
        total = z_in[k]
        for d in range(1, zn):
            total = total + z_in[d * 2 + k]
        pooled_ref[pl.ds(k * 16, 8), :] = total[:, :half]
        pooled_ref[pl.ds(k * 16 + 8, 8), :] = pltpu.roll(total, half, 1)[:, :half]

    own.wait()
    moved = flat.at[pl.ds(0, (yn * rows - 1) * span)]
    pltpu.make_async_copy(moved, moved, move_recv).wait()
    pltpu.make_async_copy(moved, moved, move_send).wait()
    sent_ids = ids.at[pl.ds(0, others)]
    pltpu.make_async_copy(sent_ids, sent_ids, ids_send).wait()
    pltpu.make_async_copy(x_rest, x_rest, x_send).wait()
    pltpu.make_async_copy(z_rest, z_rest, z_send).wait()
    for n in range(chunks):
        pair_copy(n).wait_send()


def per_device(zn, xn, column_table, bag_rows):
    rows = zn * xn
    chunks = lax.axis_size("col")
    length, half = column_table.shape
    span = length // (rows * chunks)
    f32 = jnp.float32
    dma = pltpu.SemaphoreType.DMA
    row_table, pooled = pl.pallas_call(
        functools.partial(kernel, zn, xn, span),
        out_shape=[
            jax.ShapeDtypeStruct((rows, span, half * chunks), f32),
            jax.ShapeDtypeStruct((bag_rows.shape[0], half), f32),
        ],
        in_specs=[pl.BlockSpec(memory_space=pltpu.HBM)] * 2,
        out_specs=[pl.BlockSpec(memory_space=pl.ANY), pl.BlockSpec(memory_space=pltpu.VMEM)],
        scratch_shapes=[
            pltpu.VMEM((2 * half, length), f32),
            pltpu.VMEM((length + 8, LANES), f32),
            pltpu.VMEM(bag_rows.shape, jnp.int32),
            pltpu.VMEM((rows * 8, LANES), jnp.int32),
            pltpu.VMEM((rows * 8, LANES), jnp.int32),
            pltpu.VMEM((2, rows * 8, LANES), f32),
            pltpu.VMEM((xn, zn, 2, 8, LANES), f32),
            pltpu.VMEM((xn, zn, 2, 8, LANES), f32),
            pltpu.VMEM((zn, 2, 8, LANES), f32),
            pltpu.VMEM((zn * 2, 8, LANES), f32),
            pltpu.SMEM((rows * 8, LANES), jnp.int32),
            dma((chunks,)), dma((chunks,)), dma((chunks,)),
            dma, dma, dma, dma, dma, dma, dma, dma, dma, dma, dma,
        ],
        compiler_params=pltpu.CompilerParams(has_side_effects=True, collective_id=0, vmem_limit_bytes=40 * 1024 * 1024),
    )(column_table.T, bag_rows)
    return row_table, pooled


def solution(mesh):
    rows = mesh.shape["row"]
    xn = 4 if rows == 32 else 2
    return jax.shard_map(
        functools.partial(per_device, rows // xn, xn),
        mesh=mesh,
        in_specs=(P("row", "col"), P("row", None)),
        out_specs=(P(None, ("col", "row"), None), P("row", "col")),
        check_vma=False,
    )
```

```python
import functools

import jax
import jax.numpy as jnp
from jax import lax
from jax.experimental import pallas as pl
from jax.experimental.pallas import tpu as pltpu
from jax.sharding import PartitionSpec as P

MESH = pl.DeviceIdType.MESH
LANES = 128
BAG_LEN = 32


def kernel(
    zn, xn, span, table_ref, bags_ref, out_ref, pooled_ref,
    raw, flat, bags, ids, near, part2, part, x_in, held, z_in, spot,
    load_sem, pair_send, pair_recv, ids_send, ids_recv, move_send, move_recv,
    x_send, x_recv, z_send, z_recv, spot_sem, own_sem, bags_sem,
):
    rows = zn * xn
    half, length = table_ref.shape
    width = rows * span
    chunks = length // width
    yn = chunks // 2
    col = lax.axis_index("col")
    row = lax.axis_index("row")
    y, core = col // 2, col % 2
    z, x = row // xn, row % xn
    sibling = y * 2 + (1 - core)
    away = sorted(range(1, zn), key=lambda d: -min(d, zn - d))

    barrier = pltpu.get_barrier_semaphore()

    def greet(c, rr):
        pl.semaphore_signal(barrier, inc=1, device_id=(c, rr), device_id_type=MESH)

    def greet_plane(i, carry):
        c = lax.rem(y + i, yn) * 2 + core
        for dx in range(xn):
            xx = lax.rem(x + dx, xn)
            for dz in away + ([0] if dx else []):
                greet(c, lax.rem(z + dz, zn) * xn + xx)
        return carry

    greet(sibling, row)
    lax.fori_loop(0, yn, greet_plane, 0)
    for dz in away:
        greet(sibling, lax.rem(z + dz, zn) * xn + x)
    for i in range(1, yn):
        greet(lax.rem(y + i, yn) * 2 + core, row)

    def load_of_pair(n):
        return n + yn if n < yn else n - yn

    def chunk_at(i, parity):
        c = lax.rem(y + i, yn) * 2 + parity
        return c, pl.ds(pl.multiple_of(c * width, LANES), width)

    def local_load(n):
        c, lanes = chunk_at(n % yn, core if n < yn else 1 - core)
        mine = pl.ds(pl.multiple_of(core * half, 8), half)
        return pltpu.make_async_copy(table_ref.at[:, lanes], raw.at[mine, lanes], load_sem.at[n])

    def pair_copy(n):
        c, lanes = chunk_at(n % yn, 1 - core if n < yn else core)
        mine = pl.ds(pl.multiple_of(core * half, 8), half)
        return pltpu.make_async_remote_copy(
            src_ref=raw.at[mine, lanes], dst_ref=raw.at[mine, lanes],
            send_sem=pair_send.at[n], recv_sem=pair_recv.at[n],
            device_id=(sibling, row), device_id_type=MESH,
        )

    load_bags = pltpu.make_async_copy(bags_ref, bags, bags_sem)
    load_bags.start()
    for n in range(yn):
        local_load(n + yn).start()
        local_load(n).start()

    load_bags.wait()
    eighth = bags.shape[0] // 4
    own_ids = pl.ds(pl.multiple_of(row * eighth, 8), eighth)
    ids[own_ids, :] = jnp.concatenate([bags[q * eighth : (q + 1) * eighth, :] for q in range(4)], axis=1)
    flat[pl.ds(length, 8), :] = jnp.zeros((8, LANES), jnp.float32)

    for n in range(chunks):
        local_load(n).wait()

    def transpose(n):
        c, lanes = chunk_at(n % yn, core if n < yn else 1 - core)
        pair_copy(n).wait_recv()

        def step(t, carry):
            at = pl.ds(pl.multiple_of(c * width + t * LANES, LANES), LANES)
            flat[at, :] = raw[:, at].T
            return carry

        lax.fori_loop(0, width // LANES, step, 0)

    def block(c, rr):
        return flat.at[pl.ds(pl.multiple_of(c * width + rr * span, 8), span)]

    landing = out_ref.at[row, :, pl.ds(pl.multiple_of(y * LANES, LANES), LANES)]

    def send_blocks(n):
        c, _ = chunk_at(n, core)

        def send(rr):
            pltpu.make_async_remote_copy(
                src_ref=block(c, rr), dst_ref=landing, send_sem=move_send, recv_sem=move_recv,
                device_id=(c, rr), device_id_type=MESH,
            ).start()

        def step(dx, carry):
            xx = lax.rem(x + dx, xn)
            for dz in away:
                send(lax.rem(z + dz, zn) * xn + xx)
            return carry

        def step_near(dx, carry):
            send(z * xn + lax.rem(x + dx, xn))
            return carry

        lax.fori_loop(0, xn, step, 0)
        lax.fori_loop(1 if n == 0 else 0, xn, step_near, 0)

    def send_ids(t, carry):
        rr = lax.rem(row + t, rows)
        pltpu.make_async_remote_copy(
            src_ref=ids.at[own_ids], dst_ref=ids.at[own_ids], send_sem=ids_send, recv_sem=ids_recv,
            device_id=(col, rr), device_id_type=MESH,
        ).start()
        return carry

    pl.semaphore_wait(barrier, yn * rows - 1 + zn)
    for n in range(chunks):
        pair_copy(n).start()
    transpose(0)
    lax.fori_loop(1, rows, send_ids, 0)
    send_blocks(0)
    for n in range(1, yn):
        transpose(n)
        if n > 1:
            send_blocks(n - 1)
    for n in range(yn, chunks):
        transpose(n)

    others = (rows - 1) * eighth
    pltpu.make_async_copy(ids.at[pl.ds(0, others)], ids.at[pl.ds(0, others)], ids_recv).wait()
    every = ids[...]
    every = jnp.where(every // length == row, every % length, length)
    near[...] = jnp.where(core == 0, every, pltpu.roll(every, LANES // 2, 1))
    to_scalar = pltpu.make_async_copy(near, spot, spot_sem)
    to_scalar.start()
    to_scalar.wait()

    def gather(t, carry):
        for q in range(2):
            sums = [None] * 4
            for l in range(BAG_LEN):
                at = spot[t, q * BAG_LEN + l]
                value = flat[pl.ds(at, 1), :]
                sums[l % 4] = value if sums[l % 4] is None else sums[l % 4] + value
            part2[q, pl.ds(t, 1), :] = (sums[0] + sums[1]) + (sums[2] + sums[3])
        return carry

    lax.fori_loop(0, rows * eighth, gather, 0)

    low = lax.broadcasted_iota(jnp.int32, (8, LANES), 1) < half

    def split(s, carry):
        at = pl.ds(pl.multiple_of(s * 8, 8), 8)
        first, second = part2[0, at, :], part2[1, at, :]
        part[s % xn, s // xn, 0] = jnp.where(low, first, pltpu.roll(second, half, 1))
        part[s % xn, s // xn, 1] = jnp.where(low, pltpu.roll(first, half, 1), second)
        return carry

    lax.fori_loop(0, rows, split, 0)

    for d in range(1, xn):
        xx = lax.rem(x + d, xn)
        pltpu.make_async_remote_copy(
            src_ref=part.at[xx], dst_ref=x_in.at[x], send_sem=x_send, recv_sem=x_recv,
            device_id=(col, z * xn + xx), device_id_type=MESH,
        ).start()
    x_rest = part.at[pl.ds(0, xn - 1)]
    pltpu.make_async_copy(x_rest, x_rest, x_recv).wait()
    total = part[x]
    for d in range(1, xn):
        total = total + x_in[lax.rem(x + d, xn)]
    held[...] = total

    for d in range(zn):
        zz = lax.rem(z + d, zn)
        for e in range(2):
            if d == 0 and e == 0:
                continue
            kk = core if e == 0 else 1 - core
            pltpu.make_async_remote_copy(
                src_ref=held.at[zz, kk], dst_ref=z_in.at[z * 2 + core], send_sem=z_send, recv_sem=z_recv,
                device_id=(y * 2 + kk, zz * xn + x), device_id_type=MESH,
            ).start()
    send_blocks(yn - 1)
    own = pltpu.make_async_copy(block(col, row), landing, own_sem)
    own.start()
    z_in[z * 2 + core] = held[z, core]
    z_rest = z_in.at[pl.ds(0, 2 * zn - 1)]
    pltpu.make_async_copy(z_rest, z_rest, z_recv).wait()
    for k in range(2):
        total = z_in[k]
        for d in range(1, zn):
            total = total + z_in[d * 2 + k]
        pooled_ref[pl.ds(k * 16, 8), :] = total[:, :half]
        pooled_ref[pl.ds(k * 16 + 8, 8), :] = pltpu.roll(total, half, 1)[:, :half]

    own.wait()
    moved = flat.at[pl.ds(0, (yn * rows - 1) * span)]
    pltpu.make_async_copy(moved, moved, move_recv).wait()
    pltpu.make_async_copy(moved, moved, move_send).wait()
    sent_ids = ids.at[pl.ds(0, others)]
    pltpu.make_async_copy(sent_ids, sent_ids, ids_send).wait()
    pltpu.make_async_copy(x_rest, x_rest, x_send).wait()
    pltpu.make_async_copy(z_rest, z_rest, z_send).wait()
    for n in range(chunks):
        pair_copy(n).wait_send()


def per_device(zn, xn, column_table, bag_rows):
    rows = zn * xn
    chunks = lax.axis_size("col")
    length, half = column_table.shape
    span = length // (rows * chunks)
    f32 = jnp.float32
    dma = pltpu.SemaphoreType.DMA
    row_table, pooled = pl.pallas_call(
        functools.partial(kernel, zn, xn, span),
        out_shape=[
            pltpu.VMEM((rows, span, half * chunks), f32),
            pltpu.VMEM((bag_rows.shape[0], half), f32),
        ],
        in_specs=[pl.BlockSpec(memory_space=pltpu.HBM)] * 2,
        out_specs=[pl.BlockSpec(memory_space=pl.ANY), pl.BlockSpec(memory_space=pltpu.VMEM)],
        scratch_shapes=[
            pltpu.VMEM((2 * half, length), f32),
            pltpu.VMEM((length + 8, LANES), f32),
            pltpu.VMEM(bag_rows.shape, jnp.int32),
            pltpu.VMEM((rows * 8, LANES), jnp.int32),
            pltpu.VMEM((rows * 8, LANES), jnp.int32),
            pltpu.VMEM((2, rows * 8, LANES), f32),
            pltpu.VMEM((xn, zn, 2, 8, LANES), f32),
            pltpu.VMEM((xn, zn, 2, 8, LANES), f32),
            pltpu.VMEM((zn, 2, 8, LANES), f32),
            pltpu.VMEM((zn * 2, 8, LANES), f32),
            pltpu.SMEM((rows * 8, LANES), jnp.int32),
            dma((chunks,)), dma((chunks,)), dma((chunks,)),
            dma, dma, dma, dma, dma, dma, dma, dma, dma, dma, dma,
        ],
        compiler_params=pltpu.CompilerParams(has_side_effects=True, collective_id=0, vmem_limit_bytes=56 * 1024 * 1024),
    )(column_table.T, bag_rows)
    return row_table, pooled


def solution(mesh):
    rows = mesh.shape["row"]
    xn = 4 if rows == 32 else 2
    return jax.shard_map(
        functools.partial(per_device, rows // xn, xn),
        mesh=mesh,
        in_specs=(P("row", "col"), P("row", None)),
        out_specs=(P(None, ("col", "row"), None), P("row", "col")),
        check_vma=False,
    )
```

```python
import functools

import jax
import jax.numpy as jnp
from jax import lax
from jax.experimental import pallas as pl
from jax.experimental.pallas import tpu as pltpu
from jax.sharding import PartitionSpec as P

MESH = pl.DeviceIdType.MESH
LANES = 128
BAG_LEN = 32


def apart(d, n):
    return min(d, n - d)


def kernel(
    zn, xn, span, table_ref, bags_ref, out_ref, pooled_ref,
    raw, flat, bags, ids, near, part2, part, x_in, held, z_in, spot,
    load_sem, pair_send, pair_recv, ids_send, ids_recv, move_send, move_recv,
    x_send, x_recv, z_send, z_recv, spot_sem, own_sem, bags_sem, wave,
):
    rows = zn * xn
    half, length = table_ref.shape
    width = rows * span
    chunks = length // width
    yn = chunks // 2
    col = lax.axis_index("col")
    row = lax.axis_index("row")
    y, core = col // 2, col % 2
    z, x = row // xn, row % xn
    sibling = y * 2 + (1 - core)
    order = sorted(range(yn), key=lambda d: apart(d, yn))

    def load_of_pair(n):
        return n + yn if n < yn else n - yn

    def chunk_at(i, parity):
        c = lax.rem(y + order[i], yn) * 2 + parity
        return c, pl.ds(pl.multiple_of(c * width, LANES), width)

    def local_load(n):
        c, lanes = chunk_at(n % yn, core if n < yn else 1 - core)
        mine = pl.ds(pl.multiple_of(core * half, 8), half)
        return pltpu.make_async_copy(table_ref.at[:, lanes], raw.at[mine, lanes], load_sem.at[n])

    def pair_copy(n):
        c, lanes = chunk_at(n % yn, 1 - core if n < yn else core)
        mine = pl.ds(pl.multiple_of(core * half, 8), half)
        return pltpu.make_async_remote_copy(
            src_ref=raw.at[mine, lanes], dst_ref=raw.at[mine, lanes],
            send_sem=pair_send.at[n], recv_sem=pair_recv.at[n],
            device_id=(sibling, row), device_id_type=MESH,
        )

    load_bags = pltpu.make_async_copy(bags_ref, bags, bags_sem)
    load_bags.start()
    for n in range(yn):
        local_load(n + yn).start()
        local_load(n).start()

    away = sorted(range(1, zn), key=lambda d: -apart(d, zn))
    beside = [(0, d) for d in range(1, xn) if apart(d, xn) == 1] + [(d, 0) for d in range(1, yn) if apart(d, yn) == 1]
    columns = [(dy, dx) for dy in range(yn) for dx in range(xn)]
    rounds = yn // 2 + xn // 2

    def device(dy, dz, dx):
        return lax.rem(y + dy, yn) * 2 + core, lax.rem(z + dz, zn) * xn + lax.rem(x + dx, xn)

    def signal(sem, to):
        pl.semaphore_signal(sem, inc=1, device_id=to, device_id_type=MESH)

    def tell(n):
        for to in [device(0, dz, 0) for dz in away] if n == 1 else [device(dy, 0, dx) for dy, dx in beside]:
            signal(wave.at[n - 1], to)

    def hear(n):
        pl.semaphore_wait(wave.at[n - 1], zn - 1 if n == 1 else len(beside))

    barrier = pltpu.get_barrier_semaphore()
    for dz in away:
        signal(barrier, device(0, dz, 0))
    for dy, dx in beside:
        signal(barrier, device(dy, 0, dx))
    signal(barrier, (sibling, row))

    load_bags.wait()
    eighth = bags.shape[0] // 4
    own_ids = pl.ds(pl.multiple_of((x * zn + z) * eighth, 8), eighth)
    line_ids = pl.ds(pl.multiple_of(x * zn * eighth, 8), zn * eighth)
    ids[own_ids, :] = jnp.concatenate([bags[q * eighth : (q + 1) * eighth, :] for q in range(4)], axis=1)
    flat[pl.ds(length, 8), :] = jnp.zeros((8, LANES), jnp.float32)

    def transpose(n):
        c, lanes = chunk_at(n % yn, core if n < yn else 1 - core)
        pair_copy(n).wait_recv()

        def step(t, carry):
            at = pl.ds(pl.multiple_of(c * width + t * LANES, LANES), LANES)
            flat[at, :] = raw[:, at].T
            return carry

        lax.fori_loop(0, width // LANES, step, 0)

    def block(c, rr):
        return flat.at[pl.ds(pl.multiple_of(c * width + rr * span, 8), span)]

    landing = out_ref.at[row, :, pl.ds(pl.multiple_of(y * LANES, LANES), LANES)]

    def send_blocks(chosen, hops):
        for dz in hops:
            for dy, dx in chosen:
                if (dy, dz, dx) == (0, 0, 0):
                    continue
                c, rr = device(dy, dz, dx)
                pltpu.make_async_remote_copy(
                    src_ref=block(c, rr), dst_ref=landing, send_sem=move_send, recv_sem=move_recv,
                    device_id=(c, rr), device_id_type=MESH,
                ).start()

    def send_ids(which, to, n):
        pltpu.make_async_remote_copy(
            src_ref=ids.at[which], dst_ref=ids.at[which], send_sem=ids_send.at[n], recv_sem=ids_recv.at[n],
            device_id=to, device_id_type=MESH,
        ).start()

    z_ids = ids.at[pl.ds(0, (zn - 1) * eighth)]
    x_ids = ids.at[pl.ds(0, (xn - 1) * zn * eighth)]

    reached = [[c for c in columns if apart(c[0], yn) + apart(c[1], xn) == n] for n in range(rounds + 1)]
    early = [c for c in reached[1] if c[0] == 0]
    late = [c for c in reached[1] if c[0] != 0]
    long_hops, short_hops = away[: (zn - 1) // 2], away[(zn - 1) // 2 :]

    pl.semaphore_wait(barrier, zn + len(beside))
    for dz in away:
        send_ids(own_ids, device(0, dz, 0), 0)
    for n in range(chunks):
        local_load(load_of_pair(n)).wait()
        pair_copy(n).start()
    transpose(0)
    tell(1)
    send_blocks([(0, 0)], long_hops)
    for n in range(1, yn):
        transpose(n)
    hear(1)
    tell(2)
    send_blocks(early, away + [0])
    pltpu.make_async_copy(z_ids, z_ids, ids_recv.at[0]).wait()
    hear(2)
    for dx in range(1, xn):
        send_ids(line_ids, device(0, 0, dx), 1)
    for n in range(2, rounds):
        tell(n + 1)
        send_blocks(reached[n], away + [0])
        hear(n + 1)
    for n in range(yn, chunks):
        transpose(n)

    pltpu.make_async_copy(x_ids, x_ids, ids_recv.at[1]).wait()
    every = ids[...]
    every = jnp.where(every // length == row, every % length, length)
    every = jnp.where(core == 0, every, pltpu.roll(every, LANES // 2, 1))
    folded = rows * eighth // 2
    front = lax.broadcasted_iota(jnp.int32, (folded, LANES), 1) < LANES // 2
    near[...] = jnp.where(front, every[:folded], pltpu.roll(every[folded:], LANES // 2, 1))
    to_scalar = pltpu.make_async_copy(near, spot, spot_sem)
    to_scalar.start()
    to_scalar.wait()

    def gather(t, carry):
        for part_of in range(2):
            for q in range(2):
                sums = [None] * 4
                for l in range(BAG_LEN):
                    at = spot[t, (part_of * 2 + q) * BAG_LEN + l]
                    value = flat[pl.ds(at, 1), :]
                    sums[l % 4] = value if sums[l % 4] is None else sums[l % 4] + value
                part2[q, pl.ds(part_of * folded + t, 1), :] = (sums[0] + sums[1]) + (sums[2] + sums[3])
        return carry

    lax.fori_loop(0, folded, gather, 0)

    low = lax.broadcasted_iota(jnp.int32, (8, LANES), 1) < half

    def split(s, carry):
        at = pl.ds(pl.multiple_of(s * 8, 8), 8)
        first, second = part2[0, at, :], part2[1, at, :]
        part[s // zn, s % zn, 0] = jnp.where(low, first, pltpu.roll(second, half, 1))
        part[s // zn, s % zn, 1] = jnp.where(low, pltpu.roll(first, half, 1), second)
        return carry

    lax.fori_loop(0, rows, split, 0)

    for d in range(1, xn):
        xx = lax.rem(x + d, xn)
        pltpu.make_async_remote_copy(
            src_ref=part.at[xx], dst_ref=x_in.at[x], send_sem=x_send, recv_sem=x_recv,
            device_id=(col, z * xn + xx), device_id_type=MESH,
        ).start()
    x_rest = part.at[pl.ds(0, xn - 1)]
    pltpu.make_async_copy(x_rest, x_rest, x_recv).wait()
    total = part[x]
    for d in range(1, xn):
        total = total + x_in[lax.rem(x + d, xn)]
    held[...] = total

    for d in range(zn):
        zz = lax.rem(z + d, zn)
        for e in range(2):
            if d == 0 and e == 0:
                continue
            kk = core if e == 0 else 1 - core
            pltpu.make_async_remote_copy(
                src_ref=held.at[zz, kk], dst_ref=z_in.at[z * 2 + core], send_sem=z_send, recv_sem=z_recv,
                device_id=(y * 2 + kk, zz * xn + x), device_id_type=MESH,
            ).start()
    send_blocks(reached[rounds], away + [0])
    send_blocks(late, away + [0])
    send_blocks([(0, 0)], short_hops)
    own = pltpu.make_async_copy(block(col, row), landing, own_sem)
    own.start()
    z_in[z * 2 + core] = held[z, core]
    z_rest = z_in.at[pl.ds(0, 2 * zn - 1)]
    pltpu.make_async_copy(z_rest, z_rest, z_recv).wait()
    for k in range(2):
        total = z_in[k]
        for d in range(1, zn):
            total = total + z_in[d * 2 + k]
        pooled_ref[pl.ds(k * 16, 8), :] = total[:, :half]
        pooled_ref[pl.ds(k * 16 + 8, 8), :] = pltpu.roll(total, half, 1)[:, :half]

    own.wait()
    moved = flat.at[pl.ds(0, (yn * rows - 1) * span)]
    pltpu.make_async_copy(moved, moved, move_recv).wait()
    pltpu.make_async_copy(moved, moved, move_send).wait()
    pltpu.make_async_copy(z_ids, z_ids, ids_send.at[0]).wait()
    pltpu.make_async_copy(x_ids, x_ids, ids_send.at[1]).wait()
    pltpu.make_async_copy(x_rest, x_rest, x_send).wait()
    pltpu.make_async_copy(z_rest, z_rest, z_send).wait()
    for n in range(chunks):
        pair_copy(n).wait_send()


def write_out(table_ref, pooled_ref, table_out, pooled_out, sems):
    table = pltpu.make_async_copy(table_ref, table_out, sems.at[0])
    pooled = pltpu.make_async_copy(pooled_ref, pooled_out, sems.at[1])
    table.start()
    pooled.start()
    table.wait()
    pooled.wait()


def per_device(zn, xn, column_table, bag_rows):
    rows = zn * xn
    chunks = lax.axis_size("col")
    length, half = column_table.shape
    span = length // (rows * chunks)
    f32 = jnp.float32
    dma = pltpu.SemaphoreType.DMA
    row_table, pooled = pl.pallas_call(
        functools.partial(kernel, zn, xn, span),
        out_shape=[
            pltpu.VMEM((rows, span, half * chunks), f32),
            pltpu.VMEM((bag_rows.shape[0], half), f32),
        ],
        in_specs=[pl.BlockSpec(memory_space=pltpu.HBM)] * 2,
        out_specs=[pl.BlockSpec(memory_space=pl.ANY), pl.BlockSpec(memory_space=pltpu.VMEM)],
        scratch_shapes=[
            pltpu.VMEM((2 * half, length), f32),
            pltpu.VMEM((length + 8, LANES), f32),
            pltpu.VMEM(bag_rows.shape, jnp.int32),
            pltpu.VMEM((rows * 8, LANES), jnp.int32),
            pltpu.VMEM((rows * 4, LANES), jnp.int32),
            pltpu.VMEM((2, rows * 8, LANES), f32),
            pltpu.VMEM((xn, zn, 2, 8, LANES), f32),
            pltpu.VMEM((xn, zn, 2, 8, LANES), f32),
            pltpu.VMEM((zn, 2, 8, LANES), f32),
            pltpu.VMEM((zn * 2, 8, LANES), f32),
            pltpu.SMEM((rows * 4, LANES), jnp.int32),
            dma((chunks,)), dma((chunks,)), dma((chunks,)),
            dma((2,)), dma((2,)), dma, dma, dma, dma, dma, dma, dma, dma, dma,
            pltpu.SemaphoreType.REGULAR((chunks // 4 + xn // 2,)),
        ],
        compiler_params=pltpu.CompilerParams(has_side_effects=True, collective_id=0, vmem_limit_bytes=56 * 1024 * 1024),
    )(column_table.T, bag_rows)
    return pl.pallas_call(
        write_out,
        out_shape=[
            jax.ShapeDtypeStruct(row_table.shape, f32),
            jax.ShapeDtypeStruct(pooled.shape, f32),
        ],
        in_specs=[pl.BlockSpec(memory_space=pl.ANY)] * 2,
        out_specs=[pl.BlockSpec(memory_space=pl.ANY)] * 2,
        scratch_shapes=[dma((2,))],
        compiler_params=pltpu.CompilerParams(vmem_limit_bytes=16 * 1024 * 1024),
    )(row_table, pooled)


def solution(mesh):
    rows = mesh.shape["row"]
    xn = 4 if rows == 32 else 2
    return jax.shard_map(
        functools.partial(per_device, rows // xn, xn),
        mesh=mesh,
        in_specs=(P("row", "col"), P("row", None)),
        out_specs=(P(None, ("col", "row"), None), P("row", "col")),
        check_vma=False,
    )
```

```python
import functools

import jax
import jax.numpy as jnp
from jax import lax
from jax.experimental import pallas as pl
from jax.experimental.pallas import tpu as pltpu
from jax.sharding import PartitionSpec as P

MESH = pl.DeviceIdType.MESH
LANES = 128
BAG_LEN = 32


def apart(d, n):
    return min(d, n - d)


def kernel(
    zn, xn, span, table_ref, bags_ref, out_ref, pooled_ref,
    raw, flat, bags, ids, near, part2, part, x_in, held, z_in, spot,
    load_sem, pair_send, pair_recv, ids_send, ids_recv, move_send, move_recv,
    x_send, x_recv, z_send, z_recv, spot_sem, own_sem, bags_sem, wave,
):
    rows = zn * xn
    half, length = table_ref.shape
    width = rows * span
    chunks = length // width
    yn = chunks // 2
    col = lax.axis_index("col")
    row = lax.axis_index("row")
    y, core = col // 2, col % 2
    z, x = row // xn, row % xn
    sibling = y * 2 + (1 - core)
    order = sorted(range(yn), key=lambda d: apart(d, yn))

    def load_of_pair(n):
        return n + yn if n < yn else n - yn

    def chunk_at(i, parity):
        c = lax.rem(y + order[i], yn) * 2 + parity
        return c, pl.ds(pl.multiple_of(c * width, LANES), width)

    def local_load(n):
        c, lanes = chunk_at(n % yn, core if n < yn else 1 - core)
        mine = pl.ds(pl.multiple_of(core * half, 8), half)
        return pltpu.make_async_copy(table_ref.at[:, lanes], raw.at[mine, lanes], load_sem.at[n])

    def pair_copy(n):
        c, lanes = chunk_at(n % yn, 1 - core if n < yn else core)
        mine = pl.ds(pl.multiple_of(core * half, 8), half)
        return pltpu.make_async_remote_copy(
            src_ref=raw.at[mine, lanes], dst_ref=raw.at[mine, lanes],
            send_sem=pair_send.at[n], recv_sem=pair_recv.at[n],
            device_id=(sibling, row), device_id_type=MESH,
        )

    load_bags = pltpu.make_async_copy(bags_ref, bags, bags_sem)
    load_bags.start()
    for n in range(yn):
        local_load(n + yn).start()
        local_load(n).start()

    away = sorted(range(1, zn), key=lambda d: -apart(d, zn))
    beside = [(0, d) for d in range(1, xn) if apart(d, xn) == 1] + [(d, 0) for d in range(1, yn) if apart(d, yn) == 1]
    columns = [(dy, dx) for dy in range(yn) for dx in range(xn)]
    rounds = yn // 2 + xn // 2

    def device(dy, dz, dx):
        return lax.rem(y + dy, yn) * 2 + core, lax.rem(z + dz, zn) * xn + lax.rem(x + dx, xn)

    def signal(sem, to):
        pl.semaphore_signal(sem, inc=1, device_id=to, device_id_type=MESH)

    def tell(n):
        for to in [device(0, dz, 0) for dz in away] if n == 1 else [device(dy, 0, dx) for dy, dx in beside]:
            signal(wave.at[n - 1], to)

    def hear(n):
        pl.semaphore_wait(wave.at[n - 1], zn - 1 if n == 1 else len(beside))

    barrier = pltpu.get_barrier_semaphore()
    for dz in away:
        signal(barrier, device(0, dz, 0))
    for dy, dx in beside:
        signal(barrier, device(dy, 0, dx))
    signal(barrier, (sibling, row))

    load_bags.wait()
    eighth = bags.shape[0] // 4
    own_ids = pl.ds(pl.multiple_of((x * zn + z) * eighth, 8), eighth)
    line_ids = pl.ds(pl.multiple_of(x * zn * eighth, 8), zn * eighth)
    ids[own_ids, :] = jnp.concatenate([bags[q * eighth : (q + 1) * eighth, :] for q in range(4)], axis=1)
    flat[pl.ds(length, 8), :] = jnp.zeros((8, LANES), jnp.float32)

    def transpose(n):
        c, lanes = chunk_at(n % yn, core if n < yn else 1 - core)
        pair_copy(n).wait_recv()

        def step(t, carry):
            at = pl.ds(pl.multiple_of(c * width + t * LANES, LANES), LANES)
            flat[at, :] = raw[:, at].T
            return carry

        lax.fori_loop(0, width // LANES, step, 0)

    def block(c, rr):
        return flat.at[pl.ds(pl.multiple_of(c * width + rr * span, 8), span)]

    landing = out_ref.at[row, :, pl.ds(pl.multiple_of(y * LANES, LANES), LANES)]

    def send_blocks(chosen, hops):
        for dz in hops:
            for dy, dx in chosen:
                if (dy, dz, dx) == (0, 0, 0):
                    continue
                c, rr = device(dy, dz, dx)
                pltpu.make_async_remote_copy(
                    src_ref=block(c, rr), dst_ref=landing, send_sem=move_send, recv_sem=move_recv,
                    device_id=(c, rr), device_id_type=MESH,
                ).start()

    def send_ids(which, to, n):
        pltpu.make_async_remote_copy(
            src_ref=ids.at[which], dst_ref=ids.at[which], send_sem=ids_send.at[n], recv_sem=ids_recv.at[n],
            device_id=to, device_id_type=MESH,
        ).start()

    z_ids = ids.at[pl.ds(0, (zn - 1) * eighth)]
    x_ids = ids.at[pl.ds(0, (xn - 1) * zn * eighth)]

    reached = [[c for c in columns if apart(c[0], yn) + apart(c[1], xn) == n] for n in range(rounds + 1)]
    early = [c for c in reached[1] if c[0] == 0]
    late = [c for c in reached[1] if c[0] != 0]
    long_hops, short_hops = away[: (zn - 1) // 2], away[(zn - 1) // 2 :]

    pl.semaphore_wait(barrier, zn + len(beside))
    for dz in away:
        send_ids(own_ids, device(0, dz, 0), 0)
    for n in range(chunks):
        local_load(load_of_pair(n)).wait()
        pair_copy(n).start()
    transpose(0)
    tell(1)
    send_blocks([(0, 0)], long_hops)
    for n in range(1, yn):
        transpose(n)
    hear(1)
    tell(2)
    send_blocks(early, away + [0])
    pltpu.make_async_copy(z_ids, z_ids, ids_recv.at[0]).wait()
    hear(2)
    for dx in range(1, xn):
        send_ids(line_ids, device(0, 0, dx), 1)
    for n in range(2, rounds):
        tell(n + 1)
        send_blocks(reached[n], away + [0])
        hear(n + 1)
    for n in range(yn, chunks):
        transpose(n)

    send_blocks(reached[rounds], away + [0])
    send_blocks(late, away + [0])
    pltpu.make_async_copy(x_ids, x_ids, ids_recv.at[1]).wait()
    every = ids[...]
    every = jnp.where(every // length == row, every % length, length)
    every = jnp.where(core == 0, every, pltpu.roll(every, LANES // 2, 1))
    folded = rows * eighth // 2
    front = lax.broadcasted_iota(jnp.int32, (folded, LANES), 1) < LANES // 2
    near[...] = jnp.where(front, every[:folded], pltpu.roll(every[folded:], LANES // 2, 1))
    to_scalar = pltpu.make_async_copy(near, spot, spot_sem)
    to_scalar.start()
    to_scalar.wait()

    def gather(t, carry):
        for part_of in range(2):
            for q in range(2):
                sums = [None] * 4
                for l in range(BAG_LEN):
                    at = spot[t, (part_of * 2 + q) * BAG_LEN + l]
                    value = flat[pl.ds(at, 1), :]
                    sums[l % 4] = value if sums[l % 4] is None else sums[l % 4] + value
                part2[q, pl.ds(part_of * folded + t, 1), :] = (sums[0] + sums[1]) + (sums[2] + sums[3])
        return carry

    lax.fori_loop(0, folded, gather, 0)

    low = lax.broadcasted_iota(jnp.int32, (8, LANES), 1) < half

    def split(s, carry):
        at = pl.ds(pl.multiple_of(s * 8, 8), 8)
        first, second = part2[0, at, :], part2[1, at, :]
        part[s // zn, s % zn, 0] = jnp.where(low, first, pltpu.roll(second, half, 1))
        part[s // zn, s % zn, 1] = jnp.where(low, pltpu.roll(first, half, 1), second)
        return carry

    lax.fori_loop(0, rows, split, 0)

    for d in range(1, xn):
        xx = lax.rem(x + d, xn)
        pltpu.make_async_remote_copy(
            src_ref=part.at[xx], dst_ref=x_in.at[x], send_sem=x_send, recv_sem=x_recv,
            device_id=(col, z * xn + xx), device_id_type=MESH,
        ).start()
    x_rest = part.at[pl.ds(0, xn - 1)]
    pltpu.make_async_copy(x_rest, x_rest, x_recv).wait()
    total = part[x]
    for d in range(1, xn):
        total = total + x_in[lax.rem(x + d, xn)]
    held[...] = total

    for d in range(zn):
        zz = lax.rem(z + d, zn)
        for e in range(2):
            if d == 0 and e == 0:
                continue
            kk = core if e == 0 else 1 - core
            pltpu.make_async_remote_copy(
                src_ref=held.at[zz, kk], dst_ref=z_in.at[z * 2 + core], send_sem=z_send, recv_sem=z_recv,
                device_id=(y * 2 + kk, zz * xn + x), device_id_type=MESH,
            ).start()
    send_blocks([(0, 0)], short_hops)
    own = pltpu.make_async_copy(block(col, row), landing, own_sem)
    own.start()
    z_in[z * 2 + core] = held[z, core]
    z_rest = z_in.at[pl.ds(0, 2 * zn - 1)]
    pltpu.make_async_copy(z_rest, z_rest, z_recv).wait()
    for k in range(2):
        total = z_in[k]
        for d in range(1, zn):
            total = total + z_in[d * 2 + k]
        pooled_ref[pl.ds(k * 16, 8), :] = total[:, :half]
        pooled_ref[pl.ds(k * 16 + 8, 8), :] = pltpu.roll(total, half, 1)[:, :half]

    own.wait()
    moved = flat.at[pl.ds(0, (yn * rows - 1) * span)]
    pltpu.make_async_copy(moved, moved, move_recv).wait()
    pltpu.make_async_copy(moved, moved, move_send).wait()
    pltpu.make_async_copy(z_ids, z_ids, ids_send.at[0]).wait()
    pltpu.make_async_copy(x_ids, x_ids, ids_send.at[1]).wait()
    pltpu.make_async_copy(x_rest, x_rest, x_send).wait()
    pltpu.make_async_copy(z_rest, z_rest, z_send).wait()
    for n in range(chunks):
        pair_copy(n).wait_send()


def write_out(table_ref, pooled_ref, table_out, pooled_out, sems):
    table = pltpu.make_async_copy(table_ref, table_out, sems.at[0])
    pooled = pltpu.make_async_copy(pooled_ref, pooled_out, sems.at[1])
    table.start()
    pooled.start()
    table.wait()
    pooled.wait()


def per_device(zn, xn, column_table, bag_rows):
    rows = zn * xn
    chunks = lax.axis_size("col")
    length, half = column_table.shape
    span = length // (rows * chunks)
    f32 = jnp.float32
    dma = pltpu.SemaphoreType.DMA
    row_table, pooled = pl.pallas_call(
        functools.partial(kernel, zn, xn, span),
        out_shape=[
            pltpu.VMEM((rows, span, half * chunks), f32),
            pltpu.VMEM((bag_rows.shape[0], half), f32),
        ],
        in_specs=[pl.BlockSpec(memory_space=pltpu.HBM)] * 2,
        out_specs=[pl.BlockSpec(memory_space=pl.ANY), pl.BlockSpec(memory_space=pltpu.VMEM)],
        scratch_shapes=[
            pltpu.VMEM((2 * half, length), f32),
            pltpu.VMEM((length + 8, LANES), f32),
            pltpu.VMEM(bag_rows.shape, jnp.int32),
            pltpu.VMEM((rows * 8, LANES), jnp.int32),
            pltpu.VMEM((rows * 4, LANES), jnp.int32),
            pltpu.VMEM((2, rows * 8, LANES), f32),
            pltpu.VMEM((xn, zn, 2, 8, LANES), f32),
            pltpu.VMEM((xn, zn, 2, 8, LANES), f32),
            pltpu.VMEM((zn, 2, 8, LANES), f32),
            pltpu.VMEM((zn * 2, 8, LANES), f32),
            pltpu.SMEM((rows * 4, LANES), jnp.int32),
            dma((chunks,)), dma((chunks,)), dma((chunks,)),
            dma((2,)), dma((2,)), dma, dma, dma, dma, dma, dma, dma, dma, dma,
            pltpu.SemaphoreType.REGULAR((chunks // 4 + xn // 2,)),
        ],
        compiler_params=pltpu.CompilerParams(has_side_effects=True, collective_id=0, vmem_limit_bytes=56 * 1024 * 1024),
    )(column_table.T, bag_rows)
    return pl.pallas_call(
        write_out,
        out_shape=[
            jax.ShapeDtypeStruct(row_table.shape, f32),
            jax.ShapeDtypeStruct(pooled.shape, f32),
        ],
        in_specs=[pl.BlockSpec(memory_space=pl.ANY)] * 2,
        out_specs=[pl.BlockSpec(memory_space=pl.ANY)] * 2,
        scratch_shapes=[dma((2,))],
        compiler_params=pltpu.CompilerParams(vmem_limit_bytes=16 * 1024 * 1024),
    )(row_table, pooled)


def solution(mesh):
    rows = mesh.shape["row"]
    xn = 4 if rows == 32 else 2
    return jax.shard_map(
        functools.partial(per_device, rows // xn, xn),
        mesh=mesh,
        in_specs=(P("row", "col"), P("row", None)),
        out_specs=(P(None, ("col", "row"), None), P("row", "col")),
        check_vma=False,
    )
```

```python
import functools

import jax
import jax.numpy as jnp
from jax import lax
from jax.experimental import pallas as pl
from jax.experimental.pallas import tpu as pltpu
from jax.sharding import PartitionSpec as P

MESH = pl.DeviceIdType.MESH
LANES = 128
BAG_LEN = 32


def apart(d, n):
    return min(d, n - d)


def mate(v, m, n):
    if m == 0:
        return v
    if m == n - 1:
        return n - 1 - v
    return v + 1 - 2 * lax.rem(v, 2) if m == 1 else lax.rem(v + 2, n)


def kernel(
    zn, xn, span, table_ref, bags_ref, out_ref, pooled_ref,
    raw, flat, bags, ids, near, part2, part, x_in, held, z_in, spot,
    load_sem, pair_send, pair_recv, ids_send, ids_recv, move_send, move_recv,
    x_send, x_recv, z_send, z_recv, spot_sem, own_sem, bags_sem, wave,
):
    rows = zn * xn
    half, length = table_ref.shape
    width = rows * span
    chunks = length // width
    yn = chunks // 2
    col = lax.axis_index("col")
    row = lax.axis_index("row")
    y, core = col // 2, col % 2
    z, x = row // xn, row % xn
    sibling = y * 2 + (1 - core)
    order = sorted(range(yn), key=lambda m: (m > 0, m != yn - 1, m))

    def load_of_pair(n):
        return n + yn if n < yn else n - yn

    def chunk_at(i, parity):
        c = mate(y, order[i], yn) * 2 + parity
        return c, pl.ds(pl.multiple_of(c * width, LANES), width)

    def local_load(n):
        c, lanes = chunk_at(n % yn, core if n < yn else 1 - core)
        mine = pl.ds(pl.multiple_of(core * half, 8), half)
        return pltpu.make_async_copy(table_ref.at[:, lanes], raw.at[mine, lanes], load_sem.at[n])

    def pair_copy(n):
        c, lanes = chunk_at(n % yn, 1 - core if n < yn else core)
        mine = pl.ds(pl.multiple_of(core * half, 8), half)
        return pltpu.make_async_remote_copy(
            src_ref=raw.at[mine, lanes], dst_ref=raw.at[mine, lanes],
            send_sem=pair_send.at[n], recv_sem=pair_recv.at[n],
            device_id=(sibling, row), device_id_type=MESH,
        )

    load_bags = pltpu.make_async_copy(bags_ref, bags, bags_sem)
    load_bags.start()
    for n in range(yn):
        local_load(n + yn).start()
        local_load(n).start()

    away = sorted(range(1, zn), key=lambda d: -apart(d, zn))
    beside = [(0, d) for d in range(1, xn) if apart(d, xn) == 1] + [(d, 0) for d in range(1, yn) if apart(d, yn) == 1]
    columns = [(dy, dx) for dy in range(yn) for dx in range(xn)]
    rounds = yn // 2 + xn // 2

    def device(dy, dz, dx):
        return lax.rem(y + dy, yn) * 2 + core, lax.rem(z + dz, zn) * xn + lax.rem(x + dx, xn)

    def signal(sem, to):
        pl.semaphore_signal(sem, inc=1, device_id=to, device_id_type=MESH)

    def tell(n):
        for to in [device(0, dz, 0) for dz in away] if n == 1 else [device(dy, 0, dx) for dy, dx in beside]:
            signal(wave.at[n - 1], to)

    def hear(n):
        pl.semaphore_wait(wave.at[n - 1], zn - 1 if n == 1 else len(beside))

    barrier = pltpu.get_barrier_semaphore()
    for dz in away:
        signal(barrier, device(0, dz, 0))
    for dy, dx in beside:
        signal(barrier, device(dy, 0, dx))
    signal(barrier, (sibling, row))

    load_bags.wait()
    eighth = bags.shape[0] // 4
    own_ids = pl.ds(pl.multiple_of((x * zn + z) * eighth, 8), eighth)
    line_ids = pl.ds(pl.multiple_of(x * zn * eighth, 8), zn * eighth)
    ids[own_ids, :] = jnp.concatenate([bags[q * eighth : (q + 1) * eighth, :] for q in range(4)], axis=1)
    flat[pl.ds(length, 8), :] = jnp.zeros((8, LANES), jnp.float32)

    def transpose(n):
        c, lanes = chunk_at(n % yn, core if n < yn else 1 - core)
        pair_copy(n).wait_recv()

        def step(t, carry):
            at = pl.ds(pl.multiple_of(c * width + t * LANES, LANES), LANES)
            flat[at, :] = raw[:, at].T
            return carry

        lax.fori_loop(0, width // LANES, step, 0)

    def block(c, rr):
        return flat.at[pl.ds(pl.multiple_of(c * width + rr * span, 8), span)]

    landing = out_ref.at[row, :, pl.ds(pl.multiple_of(y * LANES, LANES), LANES)]

    def send_blocks(chosen, hops):
        for dz in hops:
            for my, mx in chosen:
                if (my, dz, mx) == (0, 0, 0):
                    continue
                c = mate(y, my, yn) * 2 + core
                rr = lax.rem(z + dz, zn) * xn + mate(x, mx, xn)
                pltpu.make_async_remote_copy(
                    src_ref=block(c, rr), dst_ref=landing, send_sem=move_send, recv_sem=move_recv,
                    device_id=(c, rr), device_id_type=MESH,
                ).start()

    def send_ids(which, to, n):
        pltpu.make_async_remote_copy(
            src_ref=ids.at[which], dst_ref=ids.at[which], send_sem=ids_send.at[n], recv_sem=ids_recv.at[n],
            device_id=to, device_id_type=MESH,
        ).start()

    z_ids = ids.at[pl.ds(0, (zn - 1) * eighth)]
    x_ids = ids.at[pl.ds(0, (xn - 1) * zn * eighth)]

    def hops_to(my, mx):
        return (2 if my == 2 else min(my, 1)) + (2 if mx == 2 else min(mx, 1))

    quad = [c for c in columns if max(c) < 2]
    last = [c for c in quad if hops_to(*c) == 1]
    reached = [[c for c in columns if c not in quad and hops_to(*c) == n] for n in range(rounds + 1)]
    reached[rounds] += [c for c in quad if hops_to(*c) == 2]
    long_hops, short_hops = away[: (zn - 1) // 2], away[(zn - 1) // 2 :]

    pl.semaphore_wait(barrier, zn + len(beside))
    tell(1)
    for n in range(chunks):
        local_load(load_of_pair(n)).wait()
        pair_copy(n).start()
    transpose(0)
    for dz in away:
        send_ids(own_ids, device(0, dz, 0), 0)
    send_blocks([(0, 0)], long_hops)
    for n in range(1, yn):
        transpose(n)
    hear(1)
    tell(2)
    send_blocks(reached[1], away + [0])
    pltpu.make_async_copy(z_ids, z_ids, ids_recv.at[0]).wait()
    hear(2)
    for dx in range(1, xn):
        send_ids(line_ids, device(0, 0, dx), 1)
    if rounds > 2:
        tell(3)
        send_blocks(reached[2], away + [0])
    for n in range(yn, chunks):
        transpose(n)

    pltpu.make_async_copy(x_ids, x_ids, ids_recv.at[1]).wait()
    every = ids[...]
    every = jnp.where(every // length == row, every % length, length)
    every = jnp.where(core == 0, every, pltpu.roll(every, LANES // 2, 1))
    fold = zn * eighth // 2
    front = lax.broadcasted_iota(jnp.int32, (fold, LANES), 1) < LANES // 2
    for d in range(xn):
        upper, lower = every[d * 2 * fold : (d * 2 + 1) * fold], every[(d * 2 + 1) * fold : (d * 2 + 2) * fold]
        near[d * fold : (d + 1) * fold, :] = jnp.where(front, upper, pltpu.roll(lower, LANES // 2, 1))
    to_scalar = pltpu.make_async_copy(near, spot, spot_sem)
    to_scalar.start()
    to_scalar.wait()

    low = lax.broadcasted_iota(jnp.int32, (8, LANES), 1) < half

    def pool(xx):
        def gather(t, carry):
            for h in range(2):
                for q in range(2):
                    sums = [None] * 4
                    for l in range(BAG_LEN):
                        at = spot[xx * fold + t, (h * 2 + q) * BAG_LEN + l]
                        value = flat[pl.ds(at, 1), :]
                        sums[l % 4] = value if sums[l % 4] is None else sums[l % 4] + value
                    part2[q, pl.ds(h * fold + t, 1), :] = (sums[0] + sums[1]) + (sums[2] + sums[3])
            return carry

        lax.fori_loop(0, fold, gather, 0)

        for s in range(zn):
            first, second = part2[0, s * 8 : s * 8 + 8, :], part2[1, s * 8 : s * 8 + 8, :]
            part[xx, s, 0] = jnp.where(low, first, pltpu.roll(second, half, 1))
            part[xx, s, 1] = jnp.where(low, pltpu.roll(first, half, 1), second)

    def send_part(d):
        xx = lax.rem(x + d, xn)
        pltpu.make_async_remote_copy(
            src_ref=part.at[xx], dst_ref=x_in.at[x], send_sem=x_send, recv_sem=x_recv,
            device_id=(col, z * xn + xx), device_id_type=MESH,
        ).start()

    for d in range(1, xn):
        pool(lax.rem(x + d, xn))
        n = d + 2
        if n <= rounds:
            hear(n)
            if n < rounds:
                tell(n + 1)
                send_blocks(reached[n], away + [0])
        send_part(d)
    send_blocks(reached[rounds], away + [0])
    pool(x)
    x_rest = part.at[pl.ds(0, xn - 1)]
    pltpu.make_async_copy(x_rest, x_rest, x_recv).wait()
    total = part[x]
    for d in range(1, xn):
        total = total + x_in[lax.rem(x + d, xn)]
    held[...] = total

    for d in range(zn):
        zz = lax.rem(z + d, zn)
        for e in range(2):
            if d == 0 and e == 0:
                continue
            kk = core if e == 0 else 1 - core
            pltpu.make_async_remote_copy(
                src_ref=held.at[zz, kk], dst_ref=z_in.at[z * 2 + core], send_sem=z_send, recv_sem=z_recv,
                device_id=(y * 2 + kk, zz * xn + x), device_id_type=MESH,
            ).start()
    send_blocks(last, away + [0])
    send_blocks([(0, 0)], short_hops)
    own = pltpu.make_async_copy(block(col, row), landing, own_sem)
    own.start()
    z_in[z * 2 + core] = held[z, core]
    z_rest = z_in.at[pl.ds(0, 2 * zn - 1)]
    pltpu.make_async_copy(z_rest, z_rest, z_recv).wait()
    for k in range(2):
        total = z_in[k]
        for d in range(1, zn):
            total = total + z_in[d * 2 + k]
        pooled_ref[pl.ds(k * 16, 8), :] = total[:, :half]
        pooled_ref[pl.ds(k * 16 + 8, 8), :] = pltpu.roll(total, half, 1)[:, :half]

    own.wait()
    moved = flat.at[pl.ds(0, (yn * rows - 1) * span)]
    pltpu.make_async_copy(moved, moved, move_recv).wait()
    pltpu.make_async_copy(moved, moved, move_send).wait()
    pltpu.make_async_copy(z_ids, z_ids, ids_send.at[0]).wait()
    pltpu.make_async_copy(x_ids, x_ids, ids_send.at[1]).wait()
    pltpu.make_async_copy(x_rest, x_rest, x_send).wait()
    pltpu.make_async_copy(z_rest, z_rest, z_send).wait()
    for n in range(chunks):
        pair_copy(n).wait_send()


def write_out(table_ref, pooled_ref, table_out, pooled_out, sems):
    table = pltpu.make_async_copy(table_ref, table_out, sems.at[0])
    pooled = pltpu.make_async_copy(pooled_ref, pooled_out, sems.at[1])
    table.start()
    pooled.start()
    table.wait()
    pooled.wait()


def per_device(zn, xn, column_table, bag_rows):
    rows = zn * xn
    chunks = lax.axis_size("col")
    length, half = column_table.shape
    span = length // (rows * chunks)
    f32 = jnp.float32
    dma = pltpu.SemaphoreType.DMA
    row_table, pooled = pl.pallas_call(
        functools.partial(kernel, zn, xn, span),
        out_shape=[
            pltpu.VMEM((rows, span, half * chunks), f32),
            pltpu.VMEM((bag_rows.shape[0], half), f32),
        ],
        in_specs=[pl.BlockSpec(memory_space=pltpu.HBM)] * 2,
        out_specs=[pl.BlockSpec(memory_space=pl.ANY), pl.BlockSpec(memory_space=pltpu.VMEM)],
        scratch_shapes=[
            pltpu.VMEM((2 * half, length), f32),
            pltpu.VMEM((length + 8, LANES), f32),
            pltpu.VMEM(bag_rows.shape, jnp.int32),
            pltpu.VMEM((rows * 8, LANES), jnp.int32),
            pltpu.VMEM((rows * 4, LANES), jnp.int32),
            pltpu.VMEM((2, zn * 8, LANES), f32),
            pltpu.VMEM((xn, zn, 2, 8, LANES), f32),
            pltpu.VMEM((xn, zn, 2, 8, LANES), f32),
            pltpu.VMEM((zn, 2, 8, LANES), f32),
            pltpu.VMEM((zn * 2, 8, LANES), f32),
            pltpu.SMEM((rows * 4, LANES), jnp.int32),
            dma((chunks,)), dma((chunks,)), dma((chunks,)),
            dma((2,)), dma((2,)), dma, dma, dma, dma, dma, dma, dma, dma, dma,
            pltpu.SemaphoreType.REGULAR((chunks // 4 + xn // 2,)),
        ],
        compiler_params=pltpu.CompilerParams(has_side_effects=True, collective_id=0, vmem_limit_bytes=56 * 1024 * 1024),
    )(column_table.T, bag_rows)
    return pl.pallas_call(
        write_out,
        out_shape=[
            jax.ShapeDtypeStruct(row_table.shape, f32),
            jax.ShapeDtypeStruct(pooled.shape, f32),
        ],
        in_specs=[pl.BlockSpec(memory_space=pl.ANY)] * 2,
        out_specs=[pl.BlockSpec(memory_space=pl.ANY)] * 2,
        scratch_shapes=[dma((2,))],
        compiler_params=pltpu.CompilerParams(vmem_limit_bytes=16 * 1024 * 1024),
    )(row_table, pooled)


def solution(mesh):
    rows = mesh.shape["row"]
    xn = 4 if rows == 32 else 2
    return jax.shard_map(
        functools.partial(per_device, rows // xn, xn),
        mesh=mesh,
        in_specs=(P("row", "col"), P("row", None)),
        out_specs=(P(None, ("col", "row"), None), P("row", "col")),
        check_vma=False,
    )
```

```python
import functools

import jax
import jax.numpy as jnp
from jax import lax
from jax.experimental import pallas as pl
from jax.experimental.pallas import tpu as pltpu
from jax.sharding import PartitionSpec as P

MESH = pl.DeviceIdType.MESH
LANES = 128
BAG_LEN = 32


def apart(d, n):
    return min(d, n - d)


def mate(v, m, n):
    if m == 0:
        return v
    if m == n - 1:
        return n - 1 - v
    return v + 1 - 2 * lax.rem(v, 2) if m == 1 else lax.rem(v + 2, n)


def kernel(
    zn, xn, span, table_ref, bags_ref, out_ref, pooled_ref,
    raw, flat, bags, ids, near, part2, part, x_in, held, z_in, spot,
    load_sem, pair_send, pair_recv, ids_send, ids_recv, move_send, move_recv,
    x_send, x_recv, z_send, z_recv, spot_sem, own_sem, bags_sem, wave,
):
    rows = zn * xn
    half, length = table_ref.shape
    width = rows * span
    chunks = length // width
    yn = chunks // 2
    col = lax.axis_index("col")
    row = lax.axis_index("row")
    y, core = col // 2, col % 2
    z, x = row // xn, row % xn
    sibling = y * 2 + (1 - core)
    order = sorted(range(yn), key=lambda m: (m > 0, m != yn - 1, m))

    def load_of_pair(n):
        return n + yn if n < yn else n - yn

    def chunk_at(i, parity):
        c = mate(y, order[i], yn) * 2 + parity
        return c, pl.ds(pl.multiple_of(c * width, LANES), width)

    def local_load(n):
        c, lanes = chunk_at(n % yn, core if n < yn else 1 - core)
        mine = pl.ds(pl.multiple_of(core * half, 8), half)
        return pltpu.make_async_copy(table_ref.at[:, lanes], raw.at[mine, lanes], load_sem.at[n])

    def pair_copy(n):
        c, lanes = chunk_at(n % yn, 1 - core if n < yn else core)
        mine = pl.ds(pl.multiple_of(core * half, 8), half)
        return pltpu.make_async_remote_copy(
            src_ref=raw.at[mine, lanes], dst_ref=raw.at[mine, lanes],
            send_sem=pair_send.at[n], recv_sem=pair_recv.at[n],
            device_id=(sibling, row), device_id_type=MESH,
        )

    core_bags = bags.shape[0]
    own_bags = pl.ds(pl.multiple_of(core * core_bags, 8), core_bags)
    load_bags = pltpu.make_async_copy(bags_ref.at[own_bags], bags, bags_sem)
    load_bags.start()
    for n in range(yn):
        local_load(n + yn).start()
        local_load(n).start()

    away = sorted(range(1, zn), key=lambda d: -apart(d, zn))
    beside = [(0, d) for d in range(1, xn) if apart(d, xn) == 1] + [(d, 0) for d in range(1, yn) if apart(d, yn) == 1]
    columns = [(dy, dx) for dy in range(yn) for dx in range(xn)]
    rounds = yn // 2 + xn // 2

    def device(dy, dz, dx):
        return lax.rem(y + dy, yn) * 2 + core, lax.rem(z + dz, zn) * xn + lax.rem(x + dx, xn)

    def signal(sem, to):
        pl.semaphore_signal(sem, inc=1, device_id=to, device_id_type=MESH)

    def tell(n):
        for to in [device(0, dz, 0) for dz in away] if n == 1 else [device(dy, 0, dx) for dy, dx in beside]:
            signal(wave.at[n - 1], to)

    def hear(n):
        pl.semaphore_wait(wave.at[n - 1], zn - 1 if n == 1 else len(beside))

    barrier = pltpu.get_barrier_semaphore()
    for dz in away:
        signal(barrier, device(0, dz, 0))
    for dy, dx in beside:
        signal(barrier, device(dy, 0, dx))
    signal(barrier, (sibling, row))

    load_bags.wait()
    ids[x, z] = jnp.concatenate([bags[g * 4 : (g + 1) * 4, :] for g in range(core_bags // 4)], axis=1)
    flat[pl.ds(length, 8), :] = jnp.zeros((8, LANES), jnp.float32)

    def transpose(n):
        c, lanes = chunk_at(n % yn, core if n < yn else 1 - core)
        pair_copy(n).wait_recv()

        def step(t, carry):
            at = pl.ds(pl.multiple_of(c * width + t * LANES, LANES), LANES)
            flat[at, :] = raw[:, at].T
            return carry

        lax.fori_loop(0, width // LANES, step, 0)

    def block(c, rr):
        return flat.at[pl.ds(pl.multiple_of(c * width + rr * span, 8), span)]

    landing = out_ref.at[row, :, pl.ds(pl.multiple_of(y * LANES, LANES), LANES)]

    def send_blocks(chosen, hops):
        for dz in hops:
            for my, mx in chosen:
                if (my, dz, mx) == (0, 0, 0):
                    continue
                c = mate(y, my, yn) * 2 + core
                rr = lax.rem(z + dz, zn) * xn + mate(x, mx, xn)
                pltpu.make_async_remote_copy(
                    src_ref=block(c, rr), dst_ref=landing, send_sem=move_send, recv_sem=move_recv,
                    device_id=(c, rr), device_id_type=MESH,
                ).start()

    def send_last(chosen):
        for zz in range(zn):
            for my, mx in chosen:
                c = mate(y, my, yn) * 2 + core
                rr = zz * xn + mate(x, mx, xn)

                def send():
                    pltpu.make_async_remote_copy(
                        src_ref=block(c, rr), dst_ref=landing, send_sem=move_send, recv_sem=move_recv,
                        device_id=(c, rr), device_id_type=MESH,
                    ).start()

                if (my, mx) != (0, 0):
                    send()
                else:
                    dz = lax.rem(zz - z + zn, zn)
                    near_z = dz == short_hops[0]
                    for d in short_hops[1:]:
                        near_z = near_z | (dz == d)
                    pl.when(near_z)(send)

    def send_ids(held_ids, to, n):
        pltpu.make_async_remote_copy(
            src_ref=held_ids, dst_ref=held_ids, send_sem=ids_send.at[n], recv_sem=ids_recv.at[n],
            device_id=to, device_id_type=MESH,
        ).start()

    z_ids = ids.at[0, pl.ds(0, zn - 1)]
    x_ids = ids.at[pl.ds(0, xn - 1)]

    def hops_to(my, mx):
        return (2 if my == 2 else min(my, 1)) + (2 if mx == 2 else min(mx, 1))

    quad = [c for c in columns if max(c) < 2]
    last = [c for c in quad if hops_to(*c) == 1]
    reached = [[c for c in columns if c not in quad and hops_to(*c) == n] for n in range(rounds + 1)]
    reached[rounds] += [c for c in quad if hops_to(*c) == 2]
    long_hops, short_hops = away[: (zn - 1) // 2], away[(zn - 1) // 2 :]

    pl.semaphore_wait(barrier, zn + len(beside))
    tell(1)
    for n in range(chunks):
        local_load(load_of_pair(n)).wait()
        pair_copy(n).start()
    transpose(0)
    for dz in away:
        send_ids(ids.at[x, z], device(0, dz, 0), 0)
    send_blocks([(0, 0)], long_hops)
    for n in range(1, yn):
        transpose(n)
    hear(1)
    tell(2)
    send_blocks(reached[1], away + [0])
    pltpu.make_async_copy(z_ids, z_ids, ids_recv.at[0]).wait()
    hear(2)
    for dx in range(1, xn):
        send_ids(ids.at[x], device(0, 0, dx), 1)
    if rounds > 2:
        tell(3)
        send_blocks(reached[2], away + [0])
    for n in range(yn, chunks):
        transpose(n)

    pltpu.make_async_copy(x_ids, x_ids, ids_recv.at[1]).wait()
    every = ids[...]
    every = jnp.where(every // length == row, every % length, length)
    near[...] = every
    to_scalar = pltpu.make_async_copy(near, spot, spot_sem)
    to_scalar.start()
    to_scalar.wait()

    low = lax.broadcasted_iota(jnp.int32, (8, LANES), 1) < half

    def pool(xx):
        def gather(t, carry):
            owner, line = t // 4, t % 4
            for g in range(core_bags // 4):
                sums = [None] * 4
                for l in range(BAG_LEN):
                    at = spot[xx, owner, line, g * BAG_LEN + l]
                    value = flat[pl.ds(at, 1), :]
                    sums[l % 4] = value if sums[l % 4] is None else sums[l % 4] + value
                part2[g // 2, pl.ds(owner * 8 + (g % 2) * 4 + line, 1), :] = (sums[0] + sums[1]) + (sums[2] + sums[3])
            return carry

        lax.fori_loop(0, zn * 4, gather, 0)

        for s in range(zn):
            first, second = part2[0, s * 8 : s * 8 + 8, :], part2[1, s * 8 : s * 8 + 8, :]
            part[xx, s, 0] = jnp.where(low, first, pltpu.roll(second, half, 1))
            part[xx, s, 1] = jnp.where(low, pltpu.roll(first, half, 1), second)

    def send_part(d):
        xx = lax.rem(x + d, xn)
        pltpu.make_async_remote_copy(
            src_ref=part.at[xx], dst_ref=x_in.at[x], send_sem=x_send, recv_sem=x_recv,
            device_id=(col, z * xn + xx), device_id_type=MESH,
        ).start()

    for d in range(1, xn):
        pool(lax.rem(x + d, xn))
        n = d + 2
        if n <= rounds:
            hear(n)
            if n < rounds:
                tell(n + 1)
                send_blocks(reached[n], away + [0])
        send_part(d)
    send_blocks(reached[rounds], away + [0])
    pool(x)
    x_rest = part.at[pl.ds(0, xn - 1)]
    pltpu.make_async_copy(x_rest, x_rest, x_recv).wait()
    total = part[x]
    for d in range(1, xn):
        total = total + x_in[lax.rem(x + d, xn)]
    held[...] = total

    for d in range(zn):
        zz = lax.rem(z + d, zn)
        for e in range(2):
            if d == 0 and e == 0:
                continue
            kk = core if e == 0 else 1 - core
            pltpu.make_async_remote_copy(
                src_ref=held.at[zz, kk], dst_ref=z_in.at[z * 2 + core], send_sem=z_send, recv_sem=z_recv,
                device_id=(y * 2 + kk, zz * xn + x), device_id_type=MESH,
            ).start()
    send_last(last + [(0, 0)])
    own = pltpu.make_async_copy(block(col, row), landing, own_sem)
    own.start()
    z_in[z * 2 + core] = held[z, core]
    z_rest = z_in.at[pl.ds(0, 2 * zn - 1)]
    pltpu.make_async_copy(z_rest, z_rest, z_recv).wait()
    for k in range(2):
        total = z_in[k]
        for d in range(1, zn):
            total = total + z_in[d * 2 + k]
        pooled_ref[pl.ds(k * 16, 8), :] = total[:, :half]
        pooled_ref[pl.ds(k * 16 + 8, 8), :] = pltpu.roll(total, half, 1)[:, :half]

    own.wait()
    moved = flat.at[pl.ds(0, (yn * rows - 1) * span)]
    pltpu.make_async_copy(moved, moved, move_recv).wait()
    pltpu.make_async_copy(moved, moved, move_send).wait()
    pltpu.make_async_copy(z_ids, z_ids, ids_send.at[0]).wait()
    pltpu.make_async_copy(x_ids, x_ids, ids_send.at[1]).wait()
    pltpu.make_async_copy(x_rest, x_rest, x_send).wait()
    pltpu.make_async_copy(z_rest, z_rest, z_send).wait()
    for n in range(chunks):
        pair_copy(n).wait_send()


def write_out(table_ref, pooled_ref, table_out, pooled_out, sems):
    table = pltpu.make_async_copy(table_ref, table_out, sems.at[0])
    pooled = pltpu.make_async_copy(pooled_ref, pooled_out, sems.at[1])
    table.start()
    pooled.start()
    table.wait()
    pooled.wait()


def per_device(zn, xn, column_table, bag_rows):
    rows = zn * xn
    chunks = lax.axis_size("col")
    length, half = column_table.shape
    span = length // (rows * chunks)
    f32 = jnp.float32
    dma = pltpu.SemaphoreType.DMA
    row_table, pooled = pl.pallas_call(
        functools.partial(kernel, zn, xn, span),
        out_shape=[
            pltpu.VMEM((rows, span, half * chunks), f32),
            pltpu.VMEM((bag_rows.shape[0], half), f32),
        ],
        in_specs=[pl.BlockSpec(memory_space=pltpu.HBM)] * 2,
        out_specs=[pl.BlockSpec(memory_space=pl.ANY), pl.BlockSpec(memory_space=pltpu.VMEM)],
        scratch_shapes=[
            pltpu.VMEM((2 * half, length), f32),
            pltpu.VMEM((length + 8, LANES), f32),
            pltpu.VMEM((bag_rows.shape[0] // 2, BAG_LEN), jnp.int32),
            pltpu.VMEM((xn, zn, 4, LANES), jnp.int32),
            pltpu.VMEM((xn, zn, 4, LANES), jnp.int32),
            pltpu.VMEM((2, zn * 8, LANES), f32),
            pltpu.VMEM((xn, zn, 2, 8, LANES), f32),
            pltpu.VMEM((xn, zn, 2, 8, LANES), f32),
            pltpu.VMEM((zn, 2, 8, LANES), f32),
            pltpu.VMEM((zn * 2, 8, LANES), f32),
            pltpu.SMEM((xn, zn, 4, LANES), jnp.int32),
            dma((chunks,)), dma((chunks,)), dma((chunks,)),
            dma((2,)), dma((2,)), dma, dma, dma, dma, dma, dma, dma, dma, dma,
            pltpu.SemaphoreType.REGULAR((chunks // 4 + xn // 2,)),
        ],
        compiler_params=pltpu.CompilerParams(has_side_effects=True, collective_id=0, vmem_limit_bytes=56 * 1024 * 1024),
    )(column_table.T, bag_rows)
    return pl.pallas_call(
        write_out,
        out_shape=[
            jax.ShapeDtypeStruct(row_table.shape, f32),
            jax.ShapeDtypeStruct(pooled.shape, f32),
        ],
        in_specs=[pl.BlockSpec(memory_space=pl.ANY)] * 2,
        out_specs=[pl.BlockSpec(memory_space=pl.ANY)] * 2,
        scratch_shapes=[dma((2,))],
        compiler_params=pltpu.CompilerParams(vmem_limit_bytes=16 * 1024 * 1024),
    )(row_table, pooled)


def solution(mesh):
    rows = mesh.shape["row"]
    xn = 4 if rows == 32 else 2
    return jax.shard_map(
        functools.partial(per_device, rows // xn, xn),
        mesh=mesh,
        in_specs=(P("row", "col"), P("row", None)),
        out_specs=(P(None, ("col", "row"), None), P("row", "col")),
        check_vma=False,
    )
```

```python
import functools

import jax
import jax.numpy as jnp
from jax import lax
from jax.experimental import pallas as pl
from jax.experimental.pallas import tpu as pltpu
from jax.sharding import PartitionSpec as P

MESH = pl.DeviceIdType.MESH
LANES = 128
BAG_LEN = 32


def apart(d, n):
    return min(d, n - d)


def mate(v, m, n):
    if m == 0:
        return v
    if m == n - 1:
        return n - 1 - v
    return v + 1 - 2 * lax.rem(v, 2) if m == 1 else lax.rem(v + 2, n)


def kernel(
    zn, xn, span, table_ref, bags_ref, out_ref, pooled_ref,
    raw, flat, bags, ids, near, part2, part, x_in, held, z_in, spot,
    load_sem, pair_send, pair_recv, ids_send, ids_recv, move_send, move_recv,
    x_send, x_recv, z_send, z_recv, spot_sem, own_sem, bags_sem, wave,
):
    rows = zn * xn
    half, length = table_ref.shape
    width = rows * span
    chunks = length // width
    yn = chunks // 2
    col = lax.axis_index("col")
    row = lax.axis_index("row")
    y, core = col // 2, col % 2
    z, x = row // xn, row % xn
    sibling = y * 2 + (1 - core)
    order = sorted(range(yn), key=lambda m: (m > 0, m != yn - 1, m))

    def load_of_pair(n):
        return n + yn if n < yn else n - yn

    def chunk_at(i, parity):
        c = mate(y, order[i], yn) * 2 + parity
        return c, pl.ds(pl.multiple_of(c * width, LANES), width)

    def local_load(n):
        c, lanes = chunk_at(n % yn, core if n < yn else 1 - core)
        mine = pl.ds(pl.multiple_of(core * half, 8), half)
        return pltpu.make_async_copy(table_ref.at[:, lanes], raw.at[mine, lanes], load_sem.at[n])

    def pair_copy(n):
        c, lanes = chunk_at(n % yn, 1 - core if n < yn else core)
        mine = pl.ds(pl.multiple_of(core * half, 8), half)
        return pltpu.make_async_remote_copy(
            src_ref=raw.at[mine, lanes], dst_ref=raw.at[mine, lanes],
            send_sem=pair_send.at[n], recv_sem=pair_recv.at[n],
            device_id=(sibling, row), device_id_type=MESH,
        )

    core_bags = bags.shape[0]
    own_bags = pl.ds(pl.multiple_of(core * core_bags, 8), core_bags)
    load_bags = pltpu.make_async_copy(bags_ref.at[own_bags], bags, bags_sem)
    for n in range(yn):
        local_load(load_of_pair(n)).start()
    load_bags.start()
    for n in range(yn):
        local_load(n).start()

    away = sorted(range(1, zn), key=lambda d: -apart(d, zn))
    beside = [(0, d) for d in range(1, xn) if apart(d, xn) == 1] + [(d, 0) for d in range(1, yn) if apart(d, yn) == 1]
    columns = [(dy, dx) for dy in range(yn) for dx in range(xn)]
    rounds = yn // 2 + xn // 2

    def device(dy, dz, dx):
        return lax.rem(y + dy, yn) * 2 + core, lax.rem(z + dz, zn) * xn + lax.rem(x + dx, xn)

    def signal(sem, to):
        pl.semaphore_signal(sem, inc=1, device_id=to, device_id_type=MESH)

    def tell(n):
        for dy, dx in beside:
            signal(wave.at[n - 1], device(dy, 0, dx))

    def hear(n):
        pl.semaphore_wait(wave.at[n - 1], len(beside))

    barrier = pltpu.get_barrier_semaphore()
    for dz in away:
        signal(barrier, device(0, dz, 0))
    for dy, dx in beside:
        signal(barrier, device(dy, 0, dx))
    signal(barrier, (sibling, row))

    load_bags.wait()
    ids[x, z] = jnp.concatenate([bags[g * 4 : (g + 1) * 4, :] for g in range(core_bags // 4)], axis=1)
    flat[pl.ds(length, 8), :] = jnp.zeros((8, LANES), jnp.float32)

    def transpose(n):
        c, lanes = chunk_at(n % yn, core if n < yn else 1 - core)
        pair_copy(n).wait_recv()

        def step(t, carry):
            at = pl.ds(pl.multiple_of(c * width + t * LANES, LANES), LANES)
            flat[at, :] = raw[:, at].T
            return carry

        lax.fori_loop(0, width // LANES, step, 0)

    def block(c, rr):
        return flat.at[pl.ds(pl.multiple_of(c * width + rr * span, 8), span)]

    landing = out_ref.at[row, :, pl.ds(pl.multiple_of(y * LANES, LANES), LANES)]

    def send_blocks(chosen, hops):
        for dz in hops:
            for my, mx in chosen:
                if (my, dz, mx) == (0, 0, 0):
                    continue
                c = mate(y, my, yn) * 2 + core
                rr = lax.rem(z + dz, zn) * xn + mate(x, mx, xn)
                pltpu.make_async_remote_copy(
                    src_ref=block(c, rr), dst_ref=landing, send_sem=move_send, recv_sem=move_recv,
                    device_id=(c, rr), device_id_type=MESH,
                ).start()

    def send_last(chosen):
        for zz in range(zn):
            for my, mx in chosen:
                c = mate(y, my, yn) * 2 + core
                rr = zz * xn + mate(x, mx, xn)

                def send():
                    pltpu.make_async_remote_copy(
                        src_ref=block(c, rr), dst_ref=landing, send_sem=move_send, recv_sem=move_recv,
                        device_id=(c, rr), device_id_type=MESH,
                    ).start()

                if (my, mx) != (0, 0):
                    send()
                else:
                    dz = lax.rem(zz - z + zn, zn)
                    near_z = dz == short_hops[0]
                    for d in short_hops[1:]:
                        near_z = near_z | (dz == d)
                    pl.when(near_z)(send)

    def send_ids(held_ids, to, n):
        pltpu.make_async_remote_copy(
            src_ref=held_ids, dst_ref=held_ids, send_sem=ids_send.at[n], recv_sem=ids_recv.at[n],
            device_id=to, device_id_type=MESH,
        ).start()

    z_ids = ids.at[0, pl.ds(0, zn - 1)]
    x_ids = ids.at[pl.ds(0, xn - 1)]

    def hops_to(my, mx):
        return (2 if my == 2 else min(my, 1)) + (2 if mx == 2 else min(mx, 1))

    quad = [c for c in columns if max(c) < 2]
    last = [c for c in quad if hops_to(*c) == 1]
    reached = [[c for c in columns if c not in quad and hops_to(*c) == n] for n in range(rounds + 1)]
    reached[rounds] += [c for c in quad if hops_to(*c) == 2]
    long_hops, short_hops = away[: (zn - 1) // 2], away[(zn - 1) // 2 :]

    pl.semaphore_wait(barrier, zn + len(beside))
    tell(1)
    for n in range(chunks):
        local_load(load_of_pair(n)).wait()
        pair_copy(n).start()
    transpose(0)
    for dz in away:
        send_ids(ids.at[x, z], device(0, dz, 0), 0)
    send_blocks([(0, 0)], long_hops)
    transpose(1)
    hear(1)
    tell(2)
    send_blocks(reached[1], away + [0])
    for n in range(2, yn):
        transpose(n)
    pltpu.make_async_copy(z_ids, z_ids, ids_recv.at[0]).wait()
    hear(2)
    for dx in range(1, xn):
        send_ids(ids.at[x], device(0, 0, dx), 1)
    if rounds > 2:
        tell(3)
        send_blocks(reached[2], away + [0])
    for n in range(yn, chunks):
        transpose(n)

    pltpu.make_async_copy(x_ids, x_ids, ids_recv.at[1]).wait()
    every = ids[...]
    every = jnp.where(every // length == row, every % length, length)
    near[...] = every
    to_scalar = pltpu.make_async_copy(near, spot, spot_sem)
    to_scalar.start()
    to_scalar.wait()

    low = lax.broadcasted_iota(jnp.int32, (8, LANES), 1) < half

    def pool(xx):
        def gather(t, carry):
            owner, line = t // 4, t % 4
            for g in range(core_bags // 4):
                sums = [None] * 4
                for l in range(BAG_LEN):
                    at = spot[xx, owner, line, g * BAG_LEN + l]
                    value = flat[pl.ds(at, 1), :]
                    sums[l % 4] = value if sums[l % 4] is None else sums[l % 4] + value
                part2[g // 2, pl.ds(owner * 8 + (g % 2) * 4 + line, 1), :] = (sums[0] + sums[1]) + (sums[2] + sums[3])
            return carry

        lax.fori_loop(0, zn * 4, gather, 0)

        for s in range(zn):
            first, second = part2[0, s * 8 : s * 8 + 8, :], part2[1, s * 8 : s * 8 + 8, :]
            part[xx, s, 0] = jnp.where(low, first, pltpu.roll(second, half, 1))
            part[xx, s, 1] = jnp.where(low, pltpu.roll(first, half, 1), second)

    def send_part(d):
        xx = lax.rem(x + d, xn)
        pltpu.make_async_remote_copy(
            src_ref=part.at[xx], dst_ref=x_in.at[x], send_sem=x_send, recv_sem=x_recv,
            device_id=(col, z * xn + xx), device_id_type=MESH,
        ).start()

    for d in range(1, xn):
        pool(lax.rem(x + d, xn))
        n = d + 2
        if n <= rounds:
            hear(n)
            if n < rounds:
                tell(n + 1)
                send_blocks(reached[n], away + [0])
        send_part(d)
    send_blocks(reached[rounds], away + [0])
    pool(x)
    x_rest = part.at[pl.ds(0, xn - 1)]
    pltpu.make_async_copy(x_rest, x_rest, x_recv).wait()
    total = part[x]
    for d in range(1, xn):
        total = total + x_in[lax.rem(x + d, xn)]
    held[...] = total

    for d in range(zn):
        zz = lax.rem(z + d, zn)
        for e in range(2):
            if d == 0 and e == 0:
                continue
            kk = core if e == 0 else 1 - core
            pltpu.make_async_remote_copy(
                src_ref=held.at[zz, kk], dst_ref=z_in.at[z * 2 + core], send_sem=z_send, recv_sem=z_recv,
                device_id=(y * 2 + kk, zz * xn + x), device_id_type=MESH,
            ).start()
    send_last(last + [(0, 0)])
    own = pltpu.make_async_copy(block(col, row), landing, own_sem)
    own.start()
    z_in[z * 2 + core] = held[z, core]
    z_rest = z_in.at[pl.ds(0, 2 * zn - 1)]
    pltpu.make_async_copy(z_rest, z_rest, z_recv).wait()
    for k in range(2):
        total = z_in[k]
        for d in range(1, zn):
            total = total + z_in[d * 2 + k]
        pooled_ref[pl.ds(k * 16, 8), :] = total[:, :half]
        pooled_ref[pl.ds(k * 16 + 8, 8), :] = pltpu.roll(total, half, 1)[:, :half]

    own.wait()
    moved = flat.at[pl.ds(0, (yn * rows - 1) * span)]
    pltpu.make_async_copy(moved, moved, move_recv).wait()
    pltpu.make_async_copy(moved, moved, move_send).wait()
    pltpu.make_async_copy(z_ids, z_ids, ids_send.at[0]).wait()
    pltpu.make_async_copy(x_ids, x_ids, ids_send.at[1]).wait()
    pltpu.make_async_copy(x_rest, x_rest, x_send).wait()
    pltpu.make_async_copy(z_rest, z_rest, z_send).wait()
    for n in range(chunks):
        pair_copy(n).wait_send()


def write_out(table_ref, pooled_ref, table_out, pooled_out, sems):
    table = pltpu.make_async_copy(table_ref, table_out, sems.at[0])
    pooled = pltpu.make_async_copy(pooled_ref, pooled_out, sems.at[1])
    table.start()
    pooled.start()
    table.wait()
    pooled.wait()


def per_device(zn, xn, column_table, bag_rows):
    rows = zn * xn
    chunks = lax.axis_size("col")
    length, half = column_table.shape
    span = length // (rows * chunks)
    f32 = jnp.float32
    dma = pltpu.SemaphoreType.DMA
    row_table, pooled = pl.pallas_call(
        functools.partial(kernel, zn, xn, span),
        out_shape=[
            pltpu.VMEM((rows, span, half * chunks), f32),
            pltpu.VMEM((bag_rows.shape[0], half), f32),
        ],
        in_specs=[pl.BlockSpec(memory_space=pltpu.HBM)] * 2,
        out_specs=[pl.BlockSpec(memory_space=pl.ANY), pl.BlockSpec(memory_space=pltpu.VMEM)],
        scratch_shapes=[
            pltpu.VMEM((2 * half, length), f32),
            pltpu.VMEM((length + 8, LANES), f32),
            pltpu.VMEM((bag_rows.shape[0] // 2, BAG_LEN), jnp.int32),
            pltpu.VMEM((xn, zn, 4, LANES), jnp.int32),
            pltpu.VMEM((xn, zn, 4, LANES), jnp.int32),
            pltpu.VMEM((2, zn * 8, LANES), f32),
            pltpu.VMEM((xn, zn, 2, 8, LANES), f32),
            pltpu.VMEM((xn, zn, 2, 8, LANES), f32),
            pltpu.VMEM((zn, 2, 8, LANES), f32),
            pltpu.VMEM((zn * 2, 8, LANES), f32),
            pltpu.SMEM((xn, zn, 4, LANES), jnp.int32),
            dma((chunks,)), dma((chunks,)), dma((chunks,)),
            dma((2,)), dma((2,)), dma, dma, dma, dma, dma, dma, dma, dma, dma,
            pltpu.SemaphoreType.REGULAR((chunks // 4 + xn // 2,)),
        ],
        compiler_params=pltpu.CompilerParams(has_side_effects=True, collective_id=0, vmem_limit_bytes=56 * 1024 * 1024),
    )(column_table.T, bag_rows)
    return pl.pallas_call(
        write_out,
        out_shape=[
            jax.ShapeDtypeStruct(row_table.shape, f32),
            jax.ShapeDtypeStruct(pooled.shape, f32),
        ],
        in_specs=[pl.BlockSpec(memory_space=pl.ANY)] * 2,
        out_specs=[pl.BlockSpec(memory_space=pl.ANY)] * 2,
        scratch_shapes=[dma((2,))],
        compiler_params=pltpu.CompilerParams(vmem_limit_bytes=16 * 1024 * 1024),
    )(row_table, pooled)


def solution(mesh):
    rows = mesh.shape["row"]
    xn = 4 if rows == 32 else 2
    return jax.shard_map(
        functools.partial(per_device, rows // xn, xn),
        mesh=mesh,
        in_specs=(P("row", "col"), P("row", None)),
        out_specs=(P(None, ("col", "row"), None), P("row", "col")),
        check_vma=False,
    )
```

```python
import functools

import jax
import jax.numpy as jnp
from jax import lax
from jax.experimental import pallas as pl
from jax.experimental.pallas import tpu as pltpu
from jax.sharding import PartitionSpec as P

MESH = pl.DeviceIdType.MESH
LANES = 128
BAG_LEN = 32


def apart(d, n):
    return min(d, n - d)


def mate(v, m, n):
    if m == 0:
        return v
    if m == n - 1:
        return n - 1 - v
    return v + 1 - 2 * lax.rem(v, 2) if m == 1 else lax.rem(v + 2, n)


def kernel(
    zn, xn, span, table_ref, bags_ref, out_ref, pooled_ref,
    raw, flat, bags, ids, near, part2, part, x_in, held, z_in, spot,
    load_sem, pair_send, pair_recv, ids_send, ids_recv, move_send, move_recv,
    x_send, x_recv, z_send, z_recv, spot_sem, own_sem, bags_sem, wave,
):
    rows = zn * xn
    half, length = table_ref.shape
    width = rows * span
    chunks = length // width
    yn = chunks // 2
    col = lax.axis_index("col")
    row = lax.axis_index("row")
    y, core = col // 2, col % 2
    z, x = row // xn, row % xn
    sibling = y * 2 + (1 - core)
    order = sorted(range(yn), key=lambda m: (m > 0, m != yn - 1, m))

    def load_of_pair(n):
        return n + yn if n < yn else n - yn

    split = 4 if width % (4 * LANES) == 0 else 1

    def pieces(n):
        return split if n == 0 else 1

    def slot(n, p):
        return n if p == 0 else chunks + p - 1

    def chunk_at(i, parity):
        return mate(y, order[i], yn) * 2 + parity

    def lanes_of(c, p, parts):
        return pl.ds(pl.multiple_of(c * width + p * (width // parts), LANES), width // parts)

    def local_load(n):
        c = chunk_at(n % yn, core if n < yn else 1 - core)
        lanes = lanes_of(c, 0, 1)
        mine = pl.ds(pl.multiple_of(core * half, 8), half)
        return pltpu.make_async_copy(table_ref.at[:, lanes], raw.at[mine, lanes], load_sem.at[n])

    def pair_copy(n, p):
        c = chunk_at(n % yn, 1 - core if n < yn else core)
        lanes = lanes_of(c, p, pieces(n))
        mine = pl.ds(pl.multiple_of(core * half, 8), half)
        return pltpu.make_async_remote_copy(
            src_ref=raw.at[mine, lanes], dst_ref=raw.at[mine, lanes],
            send_sem=pair_send.at[slot(n, p)], recv_sem=pair_recv.at[slot(n, p)],
            device_id=(sibling, row), device_id_type=MESH,
        )

    core_bags = bags.shape[0]
    own_bags = pl.ds(pl.multiple_of(core * core_bags, 8), core_bags)
    load_bags = pltpu.make_async_copy(bags_ref.at[own_bags], bags, bags_sem)
    for n in range(yn):
        local_load(load_of_pair(n)).start()
    load_bags.start()
    for n in range(yn):
        local_load(n).start()

    away = sorted(range(1, zn), key=lambda d: -apart(d, zn))
    beside = [(0, d) for d in range(1, xn) if apart(d, xn) == 1] + [(d, 0) for d in range(1, yn) if apart(d, yn) == 1]
    columns = [(dy, dx) for dy in range(yn) for dx in range(xn)]
    rounds = yn // 2 + xn // 2

    def device(dy, dz, dx):
        return lax.rem(y + dy, yn) * 2 + core, lax.rem(z + dz, zn) * xn + lax.rem(x + dx, xn)

    def signal(sem, to):
        pl.semaphore_signal(sem, inc=1, device_id=to, device_id_type=MESH)

    def tell(n):
        for dy, dx in beside:
            signal(wave.at[n - 1], device(dy, 0, dx))

    def hear(n):
        pl.semaphore_wait(wave.at[n - 1], len(beside))

    barrier = pltpu.get_barrier_semaphore()
    for dz in away:
        signal(barrier, device(0, dz, 0))
    for dy, dx in beside:
        signal(barrier, device(dy, 0, dx))
    signal(barrier, (sibling, row))

    load_bags.wait()
    ids[x, z] = jnp.concatenate([bags[g * 4 : (g + 1) * 4, :] for g in range(core_bags // 4)], axis=1)
    flat[pl.ds(length, 8), :] = jnp.zeros((8, LANES), jnp.float32)

    def transpose(n):
        c = chunk_at(n % yn, core if n < yn else 1 - core)
        blocks = width // LANES // pieces(n)

        def step(t, carry):
            at = pl.ds(pl.multiple_of(c * width + t * LANES, LANES), LANES)
            flat[at, :] = raw[:, at].T
            return carry

        for p in range(pieces(n)):
            pair_copy(n, p).wait_recv()
            lax.fori_loop(p * blocks, (p + 1) * blocks, step, 0)

    def block(c, rr):
        return flat.at[pl.ds(pl.multiple_of(c * width + rr * span, 8), span)]

    landing = out_ref.at[row, :, pl.ds(pl.multiple_of(y * LANES, LANES), LANES)]

    def send_blocks(chosen, hops):
        for dz in hops:
            for my, mx in chosen:
                if (my, dz, mx) == (0, 0, 0):
                    continue
                c = mate(y, my, yn) * 2 + core
                rr = lax.rem(z + dz, zn) * xn + mate(x, mx, xn)
                pltpu.make_async_remote_copy(
                    src_ref=block(c, rr), dst_ref=landing, send_sem=move_send, recv_sem=move_recv,
                    device_id=(c, rr), device_id_type=MESH,
                ).start()

    def send_last(chosen):
        for zz in range(zn):
            for my, mx in chosen:
                c = mate(y, my, yn) * 2 + core
                rr = zz * xn + mate(x, mx, xn)

                def send():
                    pltpu.make_async_remote_copy(
                        src_ref=block(c, rr), dst_ref=landing, send_sem=move_send, recv_sem=move_recv,
                        device_id=(c, rr), device_id_type=MESH,
                    ).start()

                if (my, mx) != (0, 0):
                    send()
                else:
                    dz = lax.rem(zz - z + zn, zn)
                    near_z = dz == short_hops[0]
                    for d in short_hops[1:]:
                        near_z = near_z | (dz == d)
                    pl.when(near_z)(send)

    def send_ids(held_ids, to, n):
        pltpu.make_async_remote_copy(
            src_ref=held_ids, dst_ref=held_ids, send_sem=ids_send.at[n], recv_sem=ids_recv.at[n],
            device_id=to, device_id_type=MESH,
        ).start()

    z_ids = ids.at[0, pl.ds(0, zn - 1)]
    x_ids = ids.at[pl.ds(0, xn - 1)]

    def hops_to(my, mx):
        return (2 if my == 2 else min(my, 1)) + (2 if mx == 2 else min(mx, 1))

    quad = [c for c in columns if max(c) < 2]
    last = [c for c in quad if hops_to(*c) == 1]
    reached = [[c for c in columns if c not in quad and hops_to(*c) == n] for n in range(rounds + 1)]
    reached[rounds] += [c for c in quad if hops_to(*c) == 2]
    long_hops, short_hops = away[: (zn - 1) // 2], away[(zn - 1) // 2 :]

    pl.semaphore_wait(barrier, zn + len(beside))
    tell(1)
    for n in range(chunks):
        local_load(load_of_pair(n)).wait()
        for p in range(pieces(n)):
            pair_copy(n, p).start()
    transpose(0)
    for dz in away:
        send_ids(ids.at[x, z], device(0, dz, 0), 0)
    send_blocks([(0, 0)], long_hops)
    transpose(1)
    hear(1)
    tell(2)
    send_blocks(reached[1], away + [0])
    for n in range(2, yn):
        transpose(n)
    pltpu.make_async_copy(z_ids, z_ids, ids_recv.at[0]).wait()
    hear(2)
    for dx in range(1, xn):
        send_ids(ids.at[x], device(0, 0, dx), 1)
    if rounds > 2:
        tell(3)
        send_blocks(reached[2], away + [0])
    for n in range(yn, chunks):
        transpose(n)

    pltpu.make_async_copy(x_ids, x_ids, ids_recv.at[1]).wait()
    every = ids[...]
    every = jnp.where(every // length == row, every % length, length)
    near[...] = every
    to_scalar = pltpu.make_async_copy(near, spot, spot_sem)
    to_scalar.start()
    to_scalar.wait()

    low = lax.broadcasted_iota(jnp.int32, (8, LANES), 1) < half

    def pool(xx):
        def gather(t, carry):
            owner, line = t // 4, t % 4
            for g in range(core_bags // 4):
                sums = [None] * 4
                for l in range(BAG_LEN):
                    at = spot[xx, owner, line, g * BAG_LEN + l]
                    value = flat[pl.ds(at, 1), :]
                    sums[l % 4] = value if sums[l % 4] is None else sums[l % 4] + value
                part2[g // 2, pl.ds(owner * 8 + (g % 2) * 4 + line, 1), :] = (sums[0] + sums[1]) + (sums[2] + sums[3])
            return carry

        lax.fori_loop(0, zn * 4, gather, 0)

        for s in range(zn):
            first, second = part2[0, s * 8 : s * 8 + 8, :], part2[1, s * 8 : s * 8 + 8, :]
            part[xx, s, 0] = jnp.where(low, first, pltpu.roll(second, half, 1))
            part[xx, s, 1] = jnp.where(low, pltpu.roll(first, half, 1), second)

    def send_part(d):
        xx = lax.rem(x + d, xn)
        pltpu.make_async_remote_copy(
            src_ref=part.at[xx], dst_ref=x_in.at[x], send_sem=x_send, recv_sem=x_recv,
            device_id=(col, z * xn + xx), device_id_type=MESH,
        ).start()

    for d in range(1, xn):
        pool(lax.rem(x + d, xn))
        n = d + 2
        if n <= rounds:
            hear(n)
            if n < rounds:
                tell(n + 1)
                send_blocks(reached[n], away + [0])
        send_part(d)
    send_blocks(reached[rounds], away + [0])
    pool(x)
    x_rest = part.at[pl.ds(0, xn - 1)]
    pltpu.make_async_copy(x_rest, x_rest, x_recv).wait()
    total = part[x]
    for d in range(1, xn):
        total = total + x_in[lax.rem(x + d, xn)]
    held[...] = total

    for d in range(zn):
        zz = lax.rem(z + d, zn)
        for e in range(2):
            if d == 0 and e == 0:
                continue
            kk = core if e == 0 else 1 - core
            pltpu.make_async_remote_copy(
                src_ref=held.at[zz, kk], dst_ref=z_in.at[z * 2 + core], send_sem=z_send, recv_sem=z_recv,
                device_id=(y * 2 + kk, zz * xn + x), device_id_type=MESH,
            ).start()
    send_last(last + [(0, 0)])
    own = pltpu.make_async_copy(block(col, row), landing, own_sem)
    own.start()
    z_in[z * 2 + core] = held[z, core]
    z_rest = z_in.at[pl.ds(0, 2 * zn - 1)]
    pltpu.make_async_copy(z_rest, z_rest, z_recv).wait()
    for k in range(2):
        total = z_in[k]
        for d in range(1, zn):
            total = total + z_in[d * 2 + k]
        pooled_ref[pl.ds(k * 16, 8), :] = total[:, :half]
        pooled_ref[pl.ds(k * 16 + 8, 8), :] = pltpu.roll(total, half, 1)[:, :half]

    own.wait()
    moved = flat.at[pl.ds(0, (yn * rows - 1) * span)]
    pltpu.make_async_copy(moved, moved, move_recv).wait()
    pltpu.make_async_copy(moved, moved, move_send).wait()
    pltpu.make_async_copy(z_ids, z_ids, ids_send.at[0]).wait()
    pltpu.make_async_copy(x_ids, x_ids, ids_send.at[1]).wait()
    pltpu.make_async_copy(x_rest, x_rest, x_send).wait()
    pltpu.make_async_copy(z_rest, z_rest, z_send).wait()
    for n in range(chunks):
        for p in range(pieces(n)):
            pair_copy(n, p).wait_send()


def write_out(table_ref, pooled_ref, table_out, pooled_out, sems):
    table = pltpu.make_async_copy(table_ref, table_out, sems.at[0])
    pooled = pltpu.make_async_copy(pooled_ref, pooled_out, sems.at[1])
    table.start()
    pooled.start()
    table.wait()
    pooled.wait()


def per_device(zn, xn, column_table, bag_rows):
    rows = zn * xn
    chunks = lax.axis_size("col")
    length, half = column_table.shape
    span = length // (rows * chunks)
    f32 = jnp.float32
    dma = pltpu.SemaphoreType.DMA
    row_table, pooled = pl.pallas_call(
        functools.partial(kernel, zn, xn, span),
        out_shape=[
            pltpu.VMEM((rows, span, half * chunks), f32),
            pltpu.VMEM((bag_rows.shape[0], half), f32),
        ],
        in_specs=[pl.BlockSpec(memory_space=pltpu.HBM)] * 2,
        out_specs=[pl.BlockSpec(memory_space=pl.ANY), pl.BlockSpec(memory_space=pltpu.VMEM)],
        scratch_shapes=[
            pltpu.VMEM((2 * half, length), f32),
            pltpu.VMEM((length + 8, LANES), f32),
            pltpu.VMEM((bag_rows.shape[0] // 2, BAG_LEN), jnp.int32),
            pltpu.VMEM((xn, zn, 4, LANES), jnp.int32),
            pltpu.VMEM((xn, zn, 4, LANES), jnp.int32),
            pltpu.VMEM((2, zn * 8, LANES), f32),
            pltpu.VMEM((xn, zn, 2, 8, LANES), f32),
            pltpu.VMEM((xn, zn, 2, 8, LANES), f32),
            pltpu.VMEM((zn, 2, 8, LANES), f32),
            pltpu.VMEM((zn * 2, 8, LANES), f32),
            pltpu.SMEM((xn, zn, 4, LANES), jnp.int32),
            dma((chunks,)), dma((chunks + 3,)), dma((chunks + 3,)),
            dma((2,)), dma((2,)), dma, dma, dma, dma, dma, dma, dma, dma, dma,
            pltpu.SemaphoreType.REGULAR((chunks // 4 + xn // 2,)),
        ],
        compiler_params=pltpu.CompilerParams(has_side_effects=True, collective_id=0, vmem_limit_bytes=56 * 1024 * 1024),
    )(column_table.T, bag_rows)
    return pl.pallas_call(
        write_out,
        out_shape=[
            jax.ShapeDtypeStruct(row_table.shape, f32),
            jax.ShapeDtypeStruct(pooled.shape, f32),
        ],
        in_specs=[pl.BlockSpec(memory_space=pl.ANY)] * 2,
        out_specs=[pl.BlockSpec(memory_space=pl.ANY)] * 2,
        scratch_shapes=[dma((2,))],
        compiler_params=pltpu.CompilerParams(vmem_limit_bytes=16 * 1024 * 1024),
    )(row_table, pooled)


def solution(mesh):
    rows = mesh.shape["row"]
    xn = 4 if rows == 32 else 2
    return jax.shard_map(
        functools.partial(per_device, rows // xn, xn),
        mesh=mesh,
        in_specs=(P("row", "col"), P("row", None)),
        out_specs=(P(None, ("col", "row"), None), P("row", "col")),
        check_vma=False,
    )
```

```python
import functools

import jax
import jax.numpy as jnp
from jax import lax
from jax.experimental import pallas as pl
from jax.experimental.pallas import tpu as pltpu
from jax.sharding import PartitionSpec as P

MESH = pl.DeviceIdType.MESH
LANES = 128
BAG_LEN = 32


def apart(d, n):
    return min(d, n - d)


def mate(v, m, n):
    if m == 0:
        return v
    if m == n - 1:
        return n - 1 - v
    return v + 1 - 2 * lax.rem(v, 2) if m == 1 else lax.rem(v + 2, n)


def kernel(
    zn, xn, span, table_ref, bags_ref, out_ref, pooled_ref,
    raw, flat, bags, ids, near, part2, part, x_in, held, z_in, spot,
    load_sem, pair_send, pair_recv, ids_send, ids_recv, move_send, move_recv,
    x_send, x_recv, z_send, z_recv, spot_sem, own_sem, bags_sem, wave,
):
    rows = zn * xn
    half, length = table_ref.shape
    width = rows * span
    chunks = length // width
    yn = chunks // 2
    col = lax.axis_index("col")
    row = lax.axis_index("row")
    y, core = col // 2, col % 2
    z, x = row // xn, row % xn
    sibling = y * 2 + (1 - core)
    order = sorted(range(yn), key=lambda m: (m > 0, m != yn - 1, m))

    def load_of_pair(n):
        return n + yn if n < yn else n - yn

    split = 4 if width % (4 * LANES) == 0 else 1

    def pieces(n):
        return split if n == 0 else 1

    def slot(n, p):
        return n if p == 0 else chunks + p - 1

    def chunk_at(i, parity):
        return mate(y, order[i], yn) * 2 + parity

    def lanes_of(c, p, parts):
        return pl.ds(pl.multiple_of(c * width + p * (width // parts), LANES), width // parts)

    def local_load(n):
        c = chunk_at(n % yn, core if n < yn else 1 - core)
        lanes = lanes_of(c, 0, 1)
        mine = pl.ds(pl.multiple_of(core * half, 8), half)
        return pltpu.make_async_copy(table_ref.at[:, lanes], raw.at[mine, lanes], load_sem.at[n])

    def pair_copy(n, p):
        c = chunk_at(n % yn, 1 - core if n < yn else core)
        lanes = lanes_of(c, p, pieces(n))
        mine = pl.ds(pl.multiple_of(core * half, 8), half)
        return pltpu.make_async_remote_copy(
            src_ref=raw.at[mine, lanes], dst_ref=raw.at[mine, lanes],
            send_sem=pair_send.at[slot(n, p)], recv_sem=pair_recv.at[slot(n, p)],
            device_id=(sibling, row), device_id_type=MESH,
        )

    core_bags = bags.shape[0]
    own_bags = pl.ds(pl.multiple_of(core * core_bags, 8), core_bags)
    load_bags = pltpu.make_async_copy(bags_ref.at[own_bags], bags, bags_sem)
    for n in range(yn):
        local_load(load_of_pair(n)).start()
    load_bags.start()
    for n in range(yn):
        local_load(n).start()

    away = sorted(range(1, zn), key=lambda d: -apart(d, zn))
    beside = [(0, d) for d in range(1, xn) if apart(d, xn) == 1] + [(d, 0) for d in range(1, yn) if apart(d, yn) == 1]
    columns = [(dy, dx) for dy in range(yn) for dx in range(xn)]
    rounds = yn // 2 + xn // 2

    def device(dy, dz, dx):
        return lax.rem(y + dy, yn) * 2 + core, lax.rem(z + dz, zn) * xn + lax.rem(x + dx, xn)

    def signal(sem, to):
        pl.semaphore_signal(sem, inc=1, device_id=to, device_id_type=MESH)

    def tell(n):
        for dy, dx in beside:
            signal(wave.at[n - 1], device(dy, 0, dx))

    def hear(n):
        pl.semaphore_wait(wave.at[n - 1], len(beside))

    barrier = pltpu.get_barrier_semaphore()
    for dz in away:
        signal(barrier, device(0, dz, 0))
    for dy, dx in beside:
        signal(barrier, device(dy, 0, dx))
    signal(barrier, (sibling, row))

    load_bags.wait()
    ids[x, z] = jnp.concatenate([bags[g * 4 : (g + 1) * 4, :] for g in range(core_bags // 4)], axis=1)
    flat[pl.ds(length, 8), :] = jnp.zeros((8, LANES), jnp.float32)

    def transpose(n):
        c = chunk_at(n % yn, core if n < yn else 1 - core)
        blocks = width // LANES // pieces(n)

        def step(t, carry):
            at = pl.ds(pl.multiple_of(c * width + t * LANES, LANES), LANES)
            flat[at, :] = raw[:, at].T
            return carry

        for p in range(pieces(n)):
            pair_copy(n, p).wait_recv()
            lax.fori_loop(p * blocks, (p + 1) * blocks, step, 0)

    def block(c, rr):
        return flat.at[pl.ds(pl.multiple_of(c * width + rr * span, 8), span)]

    landing = out_ref.at[row, :, pl.ds(pl.multiple_of(y * LANES, LANES), LANES)]

    def send_blocks(chosen, hops):
        for dz in hops:
            for my, mx in chosen:
                if (my, dz, mx) == (0, 0, 0):
                    continue
                c = mate(y, my, yn) * 2 + core
                rr = lax.rem(z + dz, zn) * xn + mate(x, mx, xn)
                pltpu.make_async_remote_copy(
                    src_ref=block(c, rr), dst_ref=landing, send_sem=move_send, recv_sem=move_recv,
                    device_id=(c, rr), device_id_type=MESH,
                ).start()

    def send_last(chosen):
        for zz in range(zn):
            for my, mx in chosen:
                c = mate(y, my, yn) * 2 + core
                rr = zz * xn + mate(x, mx, xn)

                def send():
                    pltpu.make_async_remote_copy(
                        src_ref=block(c, rr), dst_ref=landing, send_sem=move_send, recv_sem=move_recv,
                        device_id=(c, rr), device_id_type=MESH,
                    ).start()

                if (my, mx) != (0, 0):
                    send()
                else:
                    dz = lax.rem(zz - z + zn, zn)
                    near_z = dz == short_hops[0]
                    for d in short_hops[1:]:
                        near_z = near_z | (dz == d)
                    pl.when(near_z)(send)

    def send_ids(held_ids, to, n):
        pltpu.make_async_remote_copy(
            src_ref=held_ids, dst_ref=held_ids, send_sem=ids_send.at[n], recv_sem=ids_recv.at[n],
            device_id=to, device_id_type=MESH,
        ).start()

    z_ids = ids.at[0, pl.ds(0, zn - 1)]
    x_ids = ids.at[pl.ds(0, xn - 1)]

    def hops_to(my, mx):
        return (2 if my == 2 else min(my, 1)) + (2 if mx == 2 else min(mx, 1))

    quad = [c for c in columns if max(c) < 2]
    last = [c for c in quad if hops_to(*c) == 1]
    reached = [[c for c in columns if c not in quad and hops_to(*c) == n] for n in range(rounds + 1)]
    reached[rounds] += [c for c in quad if hops_to(*c) == 2]
    long_hops, short_hops = away[: zn // 2], away[zn // 2 :]

    pl.semaphore_wait(barrier, zn + len(beside))
    tell(1)
    for n in range(chunks):
        local_load(load_of_pair(n)).wait()
        for p in range(pieces(n)):
            pair_copy(n, p).start()
    transpose(0)
    for dz in away:
        send_ids(ids.at[x, z], device(0, dz, 0), 0)
    send_blocks([(0, 0)], long_hops)
    transpose(1)
    hear(1)
    tell(2)
    send_blocks(reached[1], away + [0])
    for n in range(2, yn):
        transpose(n)
    pltpu.make_async_copy(z_ids, z_ids, ids_recv.at[0]).wait()
    hear(2)
    for dx in range(1, xn):
        send_ids(ids.at[x], device(0, 0, dx), 1)
    if rounds > 2:
        tell(3)
        send_blocks(reached[2], away + [0])
    for n in range(yn, chunks):
        transpose(n)

    pltpu.make_async_copy(x_ids, x_ids, ids_recv.at[1]).wait()
    every = ids[...]
    every = jnp.where(every // length == row, every % length, length)
    near[...] = every
    to_scalar = pltpu.make_async_copy(near, spot, spot_sem)
    to_scalar.start()
    to_scalar.wait()

    low = lax.broadcasted_iota(jnp.int32, (8, LANES), 1) < half

    def pool(xx):
        def gather(t, carry):
            owner, line = t // 4, t % 4
            for g in range(core_bags // 4):
                sums = [None] * 4
                for l in range(BAG_LEN):
                    at = spot[xx, owner, line, g * BAG_LEN + l]
                    value = flat[pl.ds(at, 1), :]
                    sums[l % 4] = value if sums[l % 4] is None else sums[l % 4] + value
                part2[g // 2, pl.ds(owner * 8 + (g % 2) * 4 + line, 1), :] = (sums[0] + sums[1]) + (sums[2] + sums[3])
            return carry

        lax.fori_loop(0, zn * 4, gather, 0)

        for s in range(zn):
            first, second = part2[0, s * 8 : s * 8 + 8, :], part2[1, s * 8 : s * 8 + 8, :]
            part[xx, s, 0] = jnp.where(low, first, pltpu.roll(second, half, 1))
            part[xx, s, 1] = jnp.where(low, pltpu.roll(first, half, 1), second)

    def send_part(d):
        xx = lax.rem(x + d, xn)
        pltpu.make_async_remote_copy(
            src_ref=part.at[xx], dst_ref=x_in.at[x], send_sem=x_send, recv_sem=x_recv,
            device_id=(col, z * xn + xx), device_id_type=MESH,
        ).start()

    for d in range(1, xn):
        pool(lax.rem(x + d, xn))
        n = d + 2
        if n <= rounds:
            hear(n)
            if n < rounds:
                tell(n + 1)
                send_blocks(reached[n], away + [0])
        send_part(d)
    send_blocks(reached[rounds], away + [0])
    pool(x)
    x_rest = part.at[pl.ds(0, xn - 1)]
    pltpu.make_async_copy(x_rest, x_rest, x_recv).wait()
    total = part[x]
    for d in range(1, xn):
        total = total + x_in[lax.rem(x + d, xn)]
    held[...] = total

    for d in away + [0]:
        zz = lax.rem(z + d, zn)
        for e in range(2):
            if d == 0 and e == 0:
                continue
            kk = core if e == 0 else 1 - core
            pltpu.make_async_remote_copy(
                src_ref=held.at[zz, kk], dst_ref=z_in.at[z * 2 + core], send_sem=z_send, recv_sem=z_recv,
                device_id=(y * 2 + kk, zz * xn + x), device_id_type=MESH,
            ).start()
    send_last(last + [(0, 0)])
    own = pltpu.make_async_copy(block(col, row), landing, own_sem)
    own.start()
    z_in[z * 2 + core] = held[z, core]
    z_rest = z_in.at[pl.ds(0, 2 * zn - 1)]
    pltpu.make_async_copy(z_rest, z_rest, z_recv).wait()
    for k in range(2):
        total = z_in[k]
        for d in range(1, zn):
            total = total + z_in[d * 2 + k]
        pooled_ref[pl.ds(k * 16, 8), :] = total[:, :half]
        pooled_ref[pl.ds(k * 16 + 8, 8), :] = pltpu.roll(total, half, 1)[:, :half]

    own.wait()
    moved = flat.at[pl.ds(0, (yn * rows - 1) * span)]
    pltpu.make_async_copy(moved, moved, move_recv).wait()
    pltpu.make_async_copy(moved, moved, move_send).wait()
    pltpu.make_async_copy(z_ids, z_ids, ids_send.at[0]).wait()
    pltpu.make_async_copy(x_ids, x_ids, ids_send.at[1]).wait()
    pltpu.make_async_copy(x_rest, x_rest, x_send).wait()
    pltpu.make_async_copy(z_rest, z_rest, z_send).wait()
    for n in range(chunks):
        for p in range(pieces(n)):
            pair_copy(n, p).wait_send()


def write_out(table_ref, pooled_ref, table_out, pooled_out, sems):
    table = pltpu.make_async_copy(table_ref, table_out, sems.at[0])
    pooled = pltpu.make_async_copy(pooled_ref, pooled_out, sems.at[1])
    table.start()
    pooled.start()
    table.wait()
    pooled.wait()


def per_device(zn, xn, column_table, bag_rows):
    rows = zn * xn
    chunks = lax.axis_size("col")
    length, half = column_table.shape
    span = length // (rows * chunks)
    f32 = jnp.float32
    dma = pltpu.SemaphoreType.DMA
    row_table, pooled = pl.pallas_call(
        functools.partial(kernel, zn, xn, span),
        out_shape=[
            pltpu.VMEM((rows, span, half * chunks), f32),
            pltpu.VMEM((bag_rows.shape[0], half), f32),
        ],
        in_specs=[pl.BlockSpec(memory_space=pltpu.HBM)] * 2,
        out_specs=[pl.BlockSpec(memory_space=pl.ANY), pl.BlockSpec(memory_space=pltpu.VMEM)],
        scratch_shapes=[
            pltpu.VMEM((2 * half, length), f32),
            pltpu.VMEM((length + 8, LANES), f32),
            pltpu.VMEM((bag_rows.shape[0] // 2, BAG_LEN), jnp.int32),
            pltpu.VMEM((xn, zn, 4, LANES), jnp.int32),
            pltpu.VMEM((xn, zn, 4, LANES), jnp.int32),
            pltpu.VMEM((2, zn * 8, LANES), f32),
            pltpu.VMEM((xn, zn, 2, 8, LANES), f32),
            pltpu.VMEM((xn, zn, 2, 8, LANES), f32),
            pltpu.VMEM((zn, 2, 8, LANES), f32),
            pltpu.VMEM((zn * 2, 8, LANES), f32),
            pltpu.SMEM((xn, zn, 4, LANES), jnp.int32),
            dma((chunks,)), dma((chunks + 3,)), dma((chunks + 3,)),
            dma((2,)), dma((2,)), dma, dma, dma, dma, dma, dma, dma, dma, dma,
            pltpu.SemaphoreType.REGULAR((chunks // 4 + xn // 2,)),
        ],
        compiler_params=pltpu.CompilerParams(has_side_effects=True, collective_id=0, vmem_limit_bytes=56 * 1024 * 1024),
    )(column_table.T, bag_rows)
    return pl.pallas_call(
        write_out,
        out_shape=[
            jax.ShapeDtypeStruct(row_table.shape, f32),
            jax.ShapeDtypeStruct(pooled.shape, f32),
        ],
        in_specs=[pl.BlockSpec(memory_space=pl.ANY)] * 2,
        out_specs=[pl.BlockSpec(memory_space=pl.ANY)] * 2,
        scratch_shapes=[dma((2,))],
        compiler_params=pltpu.CompilerParams(vmem_limit_bytes=16 * 1024 * 1024),
    )(row_table, pooled)


def solution(mesh):
    rows = mesh.shape["row"]
    xn = 4 if rows == 32 else 2
    return jax.shard_map(
        functools.partial(per_device, rows // xn, xn),
        mesh=mesh,
        in_specs=(P("row", "col"), P("row", None)),
        out_specs=(P(None, ("col", "row"), None), P("row", "col")),
        check_vma=False,
    )
```
